8 devices in a mesh: dp: 1 (over z), tx: 2 (over y), ty: 4 (over x, core).
Axes of the slice: x: 2, y: 2, z: 1, core: 2. Of those that a mesh axis runs over, the one named last changes fastest.
Arguments:
- x_in: bfloat16 [6, 729, 1152], P('dp', None, 'tx')
- ln1_gain: float32 [2, 1152], P(None, 'tx')
- ln1_bias: float32 [2, 1152], P(None, 'tx')
- w_q: bfloat16 [2, 1152, 16, 72], P(None, 'tx', 'ty')
- b_q: float32 [2, 16, 72], P(None, 'ty')
- w_k: bfloat16 [2, 1152, 16, 72], P(None, 'tx', 'ty')
- w_v: bfloat16 [2, 1152, 16, 72], P(None, 'tx', 'ty')
- b_v: float32 [2, 16, 72], P(None, 'ty')
- w_o: bfloat16 [2, 16, 72, 1152], P(None, 'ty', None, 'tx')
- b_o: float32 [2, 1152], P(None, 'tx')
- ln2_gain: float32 [2, 1152], P(None, 'tx')
- ln2_bias: float32 [2, 1152], P(None, 'tx')
- w_up: bfloat16 [2, 1152, 4304], P(None, 'tx', 'ty')
- b_up: float32 [2, 4304], P(None, 'ty')
- w_down: bfloat16 [2, 4304, 1152], P(None, 'ty', 'tx')
- b_down: float32 [2, 1152], P(None, 'tx')
Outputs:
- output: bfloat16 [6, 729, 1152], P('dp', None, 'tx')
All inputs are finite; a program needn't handle non-finite values.
Results may differ from the reference program's by a relative error of at most 0.019374.
Values are sent between devices in bfloat16 or wider.
A program may use at most 1 GiB of HBM per device.

```python
import jax
import jax.numpy as jnp
from jax import lax

IMGS = 6
N = 729
W = 1152
HEADS = 16
HEAD = 72
F = 4304
EPS = 1e-6


def setup_inputs(seed: int = 0, part: int = 0) -> dict:
    key = jax.random.key(seed)
    keys = jax.random.split(key, 16)
    act_keys = jax.random.split(jax.random.fold_in(key, part), 3)
    col_mean = 0.5 * jax.random.normal(act_keys[0], (W,), jnp.float32)
    col_scale = jnp.exp(0.5 * jax.random.normal(act_keys[1], (W,), jnp.float32))
    x_vals = jax.random.normal(act_keys[2], (IMGS, N, W), jnp.float32) * col_scale + col_mean
    w_scale = W ** -0.5
    f_scale = F ** -0.5

    def draw(index, shape, scale):
        return scale * jax.random.normal(keys[index], shape, jnp.float32)

    return {
        "x_in": x_vals.astype(jnp.bfloat16),
        "ln1_gain": 1.0 + draw(0, (2, W), 0.3),
        "ln1_bias": draw(1, (2, W), 0.3),
        "w_q": draw(2, (2, W, HEADS, HEAD), 1.7 * w_scale).astype(jnp.bfloat16),
        "b_q": draw(3, (2, HEADS, HEAD), 0.5),
        "w_k": draw(4, (2, W, HEADS, HEAD), 1.7 * w_scale).astype(jnp.bfloat16),
        "w_v": draw(5, (2, W, HEADS, HEAD), w_scale).astype(jnp.bfloat16),
        "b_v": draw(6, (2, HEADS, HEAD), 0.5),
        "w_o": draw(7, (2, HEADS, HEAD, W), w_scale).astype(jnp.bfloat16),
        "b_o": draw(8, (2, W), 0.3),
        "ln2_gain": 1.0 + draw(9, (2, W), 0.3),
        "ln2_bias": draw(10, (2, W), 0.3),
        "w_up": draw(11, (2, W, F), w_scale).astype(jnp.bfloat16),
        "b_up": draw(12, (2, F), 0.5),
        "w_down": draw(13, (2, F, W), f_scale).astype(jnp.bfloat16),
        "b_down": draw(14, (2, W), 0.3),
    }


def layer_norm(x_f, gain, shift):
    mean = jnp.mean(x_f, axis=-1, keepdims=True)
    centred = x_f - mean
    variance = jnp.mean(centred * centred, axis=-1, keepdims=True)
    return (centred * lax.rsqrt(variance + EPS) * gain + shift).astype(jnp.bfloat16)


def encoder_layer(x_img, params):
    (ln1_gain, ln1_bias, w_q, b_q, w_k, w_v, b_v, w_o, b_o,
     ln2_gain, ln2_bias, w_up, b_up, w_down, b_down) = params
    x_f = x_img.astype(jnp.float32)
    normed = layer_norm(x_f, ln1_gain, ln1_bias)
    q_proj = (jnp.dot(normed, w_q.reshape(W, W), preferred_element_type=jnp.float32) + b_q.reshape(W)).astype(jnp.bfloat16)
    k_proj = jnp.dot(normed, w_k.reshape(W, W), preferred_element_type=jnp.float32).astype(jnp.bfloat16)
    v_proj = (jnp.dot(normed, w_v.reshape(W, W), preferred_element_type=jnp.float32) + b_v.reshape(W)).astype(jnp.bfloat16)
    q_heads = q_proj.reshape(N, HEADS, HEAD).astype(jnp.float32)
    k_heads = k_proj.reshape(N, HEADS, HEAD).astype(jnp.float32)
    v_heads = v_proj.reshape(N, HEADS, HEAD).astype(jnp.float32)
    scores = jnp.einsum("qhd,khd->hqk", q_heads, k_heads) * (HEAD ** -0.5)
    attn_prob = jax.nn.softmax(scores, axis=-1).astype(jnp.bfloat16)
    attended = jnp.einsum("hqk,khd->qhd", attn_prob.astype(jnp.float32), v_heads).astype(jnp.bfloat16)
    x_mid = (x_f + jnp.dot(attended.reshape(N, W), w_o.reshape(W, W), preferred_element_type=jnp.float32) + b_o).astype(jnp.bfloat16)
    mid_f = x_mid.astype(jnp.float32)
    normed2 = layer_norm(mid_f, ln2_gain, ln2_bias)
    hidden = jax.nn.gelu(jnp.dot(normed2, w_up, preferred_element_type=jnp.float32) + b_up, approximate=True).astype(jnp.bfloat16)
    x_out = (mid_f + jnp.dot(hidden, w_down, preferred_element_type=jnp.float32) + b_down).astype(jnp.bfloat16)
    return x_out, None


def reference(x_in, ln1_gain, ln1_bias, w_q, b_q, w_k, w_v, b_v, w_o, b_o, ln2_gain, ln2_bias, w_up, b_up, w_down, b_down):
    params = (ln1_gain, ln1_bias, w_q, b_q, w_k, w_v, b_v, w_o, b_o,
              ln2_gain, ln2_bias, w_up, b_up, w_down, b_down)

    def run_image(x_img):
        x_last, _ = lax.scan(encoder_layer, x_img, params)
        return x_last

    return lax.map(run_image, x_in)
```

```python
import jax
import jax.numpy as jnp
from jax import lax
from jax.sharding import PartitionSpec as P

EPS = 1e-6
CORE = [(0, 1), (1, 0), (2, 3), (3, 2)]
CHIP = [(0, 2), (2, 0), (1, 3), (3, 1)]
ROW = [(0, 1), (1, 0)]


def norm(x_f, gain, shift):
    mean = jnp.mean(x_f, axis=-1, keepdims=True)
    centred = x_f - mean
    variance = jnp.mean(centred * centred, axis=-1, keepdims=True)
    return (centred * lax.rsqrt(variance + EPS) * gain + shift).astype(jnp.bfloat16)


def pair_order(own, other, index, axis):
    first = jnp.where(index == 0, own, other)
    second = jnp.where(index == 0, other, own)
    return jnp.concatenate([first, second], axis=axis)


def all_reduce(part):
    rows, width = part.shape
    ty = lax.axis_index("ty")
    core, chip = ty % 2, ty // 2
    padded = -(-rows // 32) * 32
    part = jnp.pad(part, ((0, padded - rows), (0, 0)))

    def scatter(value, index, pairs):
        halves = value.reshape(2, value.shape[0] // 2, width)
        got = lax.ppermute(lax.dynamic_index_in_dim(halves, 1 - index, 0, False), "ty", pairs)
        kept = lax.dynamic_index_in_dim(halves, index, 0, False)
        return (kept.astype(jnp.float32) + got.astype(jnp.float32)).astype(jnp.bfloat16)

    quarter = scatter(scatter(part, core, CORE), chip, CHIP)
    half = pair_order(quarter, lax.ppermute(quarter, "ty", CHIP), chip, 0)
    whole = pair_order(half, lax.ppermute(half, "ty", CORE), core, 0)
    return whole[:rows].astype(jnp.float32)


def solution(mesh):
    act_spec = P("dp", None, "tx")
    vec_tx = P(None, "tx")
    proj_spec = P(None, "tx", "ty", None)
    head_vec = P(None, "ty", None)
    in_specs = (act_spec, vec_tx, vec_tx, proj_spec, head_vec, proj_spec, proj_spec, head_vec,
                P(None, "ty", None, "tx"), vec_tx, vec_tx, vec_tx,
                P(None, "tx", "ty"), P(None, "ty"), P(None, "ty", "tx"), vec_tx)

    def local_fn(x_in, ln1_gain, ln1_bias, w_q, b_q, w_k, w_v, b_v, w_o, b_o, ln2_gain, ln2_bias, w_up, b_up, w_down, b_down):
        layers, half_w, heads, head = w_q.shape
        images = x_in.shape[0] // 2
        tx = lax.axis_index("tx")
        scale = head ** -0.5
        dot = lambda a, b: jnp.dot(a, b, preferred_element_type=jnp.float32)

        mine = lax.dynamic_slice_in_dim(x_in, tx * images, images)
        other = lax.ppermute(lax.dynamic_slice_in_dim(x_in, (1 - tx) * images, images), "tx", ROW)
        x_full = pair_order(mine, other, tx, 2)
        vecs = jnp.stack([ln1_gain, ln1_bias, b_o, ln2_gain, ln2_bias, b_down])
        vecs = lax.all_gather(vecs, "tx", axis=2, tiled=True)
        qkv = jnp.concatenate([w.reshape(layers, half_w, heads * head) for w in (w_q, w_k, w_v)], axis=2)
        b_qkv = jnp.concatenate([b_q.reshape(layers, -1), jnp.zeros_like(b_q).reshape(layers, -1), b_v.reshape(layers, -1)], axis=1)
        o_mat = w_o.reshape(layers, heads * head, half_w)

        def gather(w, axis):
            got = lax.ppermute(w, "tx", ROW)
            return pair_order(w, got, tx, axis)

        xs = [x_full[i] for i in range(images)]
        for layer in range(layers):
            g1, s1, bo, g2, s2, bd = [vecs[j, layer] for j in range(6)]
            wqkv = gather(qkv[layer], 0)
            wo = gather(o_mat[layer], 1)
            wup = gather(w_up[layer], 0)
            wdn = gather(w_down[layer], 1)
            mids = []
            for i in range(images):
                normed = norm(xs[i].astype(jnp.float32), g1, s1)
                proj = (dot(normed, wqkv) + b_qkv[layer]).astype(jnp.bfloat16)
                proj = proj.reshape(-1, 3, heads, head)
                scores = jnp.einsum("qhd,khd->hqk", proj[:, 0], proj[:, 1], preferred_element_type=jnp.float32) * scale
                prob = jax.nn.softmax(scores, axis=-1).astype(jnp.bfloat16)
                att = jnp.einsum("hqk,khd->qhd", prob, proj[:, 2], preferred_element_type=jnp.float32).astype(jnp.bfloat16)
                part = dot(att.reshape(-1, heads * head), wo).astype(jnp.bfloat16)
                mids.append((xs[i].astype(jnp.float32) + all_reduce(part) + bo).astype(jnp.bfloat16))
            xs = []
            for i in range(images):
                normed = norm(mids[i].astype(jnp.float32), g2, s2)
                hidden = jax.nn.gelu(dot(normed, wup) + b_up[layer], approximate=True).astype(jnp.bfloat16)
                part = dot(hidden, wdn).astype(jnp.bfloat16)
                xs.append((mids[i].astype(jnp.float32) + all_reduce(part) + bd).astype(jnp.bfloat16))
        y_full = jnp.stack(xs).reshape(images, -1, 2, half_w)
        keep = lax.dynamic_index_in_dim(y_full, tx, 2, False)
        got = lax.ppermute(lax.dynamic_index_in_dim(y_full, 1 - tx, 2, False), "tx", ROW)
        return pair_order(keep, got, tx, 0)

    return jax.shard_map(local_fn, mesh=mesh, in_specs=in_specs, out_specs=act_spec, check_vma=False)
```

```python
import functools

import jax
import jax.numpy as jnp
from jax import lax
from jax.experimental import pallas as pl
from jax.experimental.pallas import tpu as pltpu
from jax.sharding import PartitionSpec as P

EPS = 1e-6
MESH = pl.DeviceIdType.MESH
F32, BF16 = jnp.float32, jnp.bfloat16


def tn_dot(a, b):
    return lax.dot_general(a, b, (((0,), (0,)), ((), ())), preferred_element_type=F32)


def nn_dot(a, b):
    return jnp.dot(a, b, preferred_element_type=F32)


def gelu(u):
    return 0.5 * u * (1.0 + jnp.tanh(0.7978845608028654 * (u + 0.044715 * u * u * u)))


def kernel(tokens, x_hbm, vec_hbm, col_hbm, wq_hbm, wk_hbm, wv_hbm, wo_hbm, wup_hbm, wdn_hbm, out_hbm,
           xg, h, part, rd, rs, rr, acc, q3, k3, v3, att, hid, wqkv, wo, wup, wdn, vraw, uraw, vt, ut,
           loc_sem, ws_sem, wr_sem, vec_sem, col_sem, x_sem, en_s, en_r, d2_s, d2_r, rs_s, rs_r, ag_s, ag_r, ex_s, ex_r):
    dp, y, ty = lax.axis_index("dp"), lax.axis_index("tx"), lax.axis_index("ty")
    c, x = ty % 2, ty // 2
    images, width, cols = xg.shape
    half, quarter, eighth = width // 2, width // 4, width // 8
    rows_q = 3 * wq_hbm.shape[1] // 3
    head = v3.shape[1]
    heads = v3.shape[0]
    sib = (dp, y, ty + 1 - 2 * c)
    across = (dp, y, (ty + 2) % 4)
    row = (dp, 1 - y, ty)

    barrier = pltpu.get_barrier_semaphore()
    for peer in (sib, across, row):
        pl.semaphore_signal(barrier, inc=1, device_id=peer, device_id_type=MESH)

    def send(src, dst, ssem, rsem, peer):
        return pltpu.make_async_remote_copy(src_ref=src, dst_ref=dst, send_sem=ssem, recv_sem=rsem,
                                            device_id=peer, device_id_type=MESH)

    def pieces(l):
        res = []
        for t, w in enumerate((wq_hbm, wk_hbm, wv_hbm)):
            res.append((w.at[l], wqkv.at[l, y, pl.ds(rows_q * t, rows_q)]))
        res.append((wo_hbm.at[l], wo.at[l, y]))
        res.append((wup_hbm.at[l], wup.at[l, pl.ds(half * y, half)]))
        res.append((wdn_hbm.at[l], wdn.at[l, pl.ds(half * y, half)]))
        return res

    def w_local(l, n):
        src, dst = pieces(l)[n]
        return pltpu.make_async_copy(src, dst, loc_sem.at[l, n])

    def w_remote(l, n):
        src, dst = pieces(l)[n]
        return send(src, dst, ws_sem.at[l, n], wr_sem.at[l, n], row)

    def w_wait(l, ns):
        for n in ns:
            w_local(l, n).wait()
            w_remote(l, n).wait_recv()

    def mine_in(i):
        return pltpu.make_async_copy(x_hbm.at[y * images + i], xg.at[i, pl.ds(half * y, half)], x_sem.at[i])

    def entry_row(i):
        at = eighth * (2 * c + x)
        return send(x_hbm.at[(1 - y) * images + i, pl.ds(at, eighth)],
                    xg.at[i, pl.ds(half * y + at, eighth)], en_s.at[0, i], en_r.at[0, i], row)

    def entry_fwd(kind, i):
        src_x = x if kind < 3 else 1 - x
        ref = xg.at[i, pl.ds(half * (1 - y) + eighth * (2 * c + src_x), eighth)]
        return send(ref, ref, en_s.at[kind, i], en_r.at[kind, i], across if kind == 1 else sib)

    def entry(i):
        entry_row(i).wait_recv()
        entry_fwd(1, i).start()
        entry_fwd(2, i).start()
        entry_fwd(1, i).wait_recv()
        entry_fwd(3, i).start()

    def entry_done(i):
        mine_in(i).wait()
        entry_fwd(2, i).wait_recv()
        entry_fwd(3, i).wait_recv()
        entry_row(i).wait_send()
        for kind in (1, 2, 3):
            entry_fwd(kind, i).wait_send()

    def d2d(i):
        return send(part.at[pl.ds(half * (1 - c), half)], rd.at[i], d2_s.at[i], d2_r.at[i], sib)

    def scatter(i):
        return send(rs.at[i], rr.at[i], rs_s.at[i], rs_r.at[i], across)

    def gather(kind, i):
        src_x = x if kind < 2 else 1 - x
        ref = xg.at[i, pl.ds(half * c + quarter * src_x, quarter)]
        return send(ref, ref, ag_s.at[kind, i], ag_r.at[kind, i], across if kind == 0 else sib)

    def stage_b(k):
        i = k % images
        d2d(i).wait_recv()
        mine, theirs = quarter * x, quarter * (1 - x)
        acc[i] = (part[pl.ds(pl.multiple_of(half * c + mine, 16), quarter)].astype(F32)
                  + rd[i, pl.ds(pl.multiple_of(mine, 16), quarter)].astype(F32))
        rs[i] = (part[pl.ds(pl.multiple_of(half * c + theirs, 16), quarter)].astype(F32)
                 + rd[i, pl.ds(pl.multiple_of(theirs, 16), quarter)].astype(F32)).astype(BF16)
        scatter(i).start()
        d2d(i).wait_send()

    def column(ref, at, size, lane):
        block = ref[pl.ds(at, size), :]
        picked = jnp.where(lax.broadcasted_iota(jnp.int32, block.shape, 1) == lane, block, 0.0)
        return jnp.sum(picked, axis=1, keepdims=True)

    def out_piece(own_row, i, at_x):
        image = (y if own_row else 1 - y) * images + i
        return out_hbm.at[image, pl.ds(quarter * at_x, quarter)]

    def final_piece(i):
        return xg.at[i, pl.ds(half * c + quarter * x, quarter)]

    def exit_copy(kind, i):
        sems = (ex_s.at[kind, i], ex_r.at[kind, i])
        if kind == 0:
            return send(final_piece(i), out_piece(True, i, x), *sems, row)
        if kind in (1, 2):
            return send(final_piece(i), out_piece(True, i, x), *sems, across if kind == 1 else sib)
        if kind in (3, 4):
            ref = out_piece(False, i, x)
            return send(ref, ref, *sems, across if kind == 3 else sib)
        ref = out_piece(kind == 5, i, 1 - x)
        return send(ref, ref, *sems, sib)

    def exit_local(i):
        return pltpu.make_async_copy(final_piece(i), out_piece(True, i, x), x_sem.at[i])

    def stage_c(k):
        i, s = k % images, k // images
        scatter(i).wait_recv()
        at = pl.multiple_of(half * c + quarter * x, 16)
        bias = column(vt, at, quarter, 8 + s)
        new = xg[i, pl.ds(at, quarter)].astype(F32) + (acc[i] + rr[i].astype(F32)) + bias
        xg[i, pl.ds(at, quarter)] = new.astype(BF16)
        scatter(i).wait_send()

        @pl.when(s < 3)
        def _():
            gather(0, i).start()
            gather(1, i).start()

        @pl.when((s == 3) & (c == y))
        def _():
            exit_copy(1, i).start()
            exit_copy(2, i).start()
            exit_local(i).start()

        @pl.when((s == 3) & (c != y))
        def _():
            exit_copy(0, i).start()

    def stage_d(k):
        i, s = k % images, k // images

        @pl.when(s < 3)
        def _():
            gather(0, i).wait_recv()
            gather(2, i).start()

        @pl.when((s == 3) & (c == y))
        def _():
            send(final_piece(i), out_piece(False, i, x), ex_s.at[0, i], ex_r.at[0, i], row).wait_recv()
            exit_copy(3, i).start()
            exit_copy(4, i).start()
            send(final_piece(i), out_piece(True, i, 1 - x), ex_s.at[1, i], ex_r.at[1, i], across).wait_recv()
            exit_copy(5, i).start()
            piece = out_piece(False, i, 1 - x)
            send(piece, piece, ex_s.at[3, i], ex_r.at[3, i], across).wait_recv()
            exit_copy(6, i).start()

    def gather_done(k):
        i = k % images
        gather(1, i).wait_recv()
        gather(2, i).wait_recv()
        for kind in (0, 1, 2):
            gather(kind, i).wait_send()

    def norm(i, s):
        blocks = [pl.ds(b * quarter, quarter) for b in range(4)]
        total = sum(jnp.sum(xg[i, b].astype(F32), axis=0, keepdims=True) for b in blocks)
        mean = total / width
        spread = jnp.zeros_like(mean)
        for b in blocks:
            d = xg[i, b].astype(F32) - mean
            spread = spread + jnp.sum(d * d, axis=0, keepdims=True)
        inv = lax.rsqrt(spread / width + EPS)
        for n, b in enumerate(blocks):
            gain, shift = column(vt, n * quarter, quarter, s), column(vt, n * quarter, quarter, 4 + s)
            h[b] = ((xg[i, b].astype(F32) - mean) * inv * gain + shift).astype(BF16)

    def project(l, i, make):
        def body(n, _):
            hf = (1 - c) * (1 - n) + c * n
            part[pl.ds(pl.multiple_of(half * hf, 16), half)] = make(hf).astype(BF16)

            @pl.when(n == 0)
            def _():
                d2d(i).start()
            return 0
        lax.fori_loop(0, 2, body, 0)

    factor = (head ** -0.5) * 1.4426950408889634

    def attend(l, i):
        @pl.when(i == 0)
        def _():
            w_wait(l, (0, 1, 2))
        norm(i, 2 * l)
        for t, ref in enumerate((q3, k3, v3)):
            at = pl.ds(rows_q * t, rows_q)
            value = nn_dot(wqkv[l, 0, at], h[:half]) + nn_dot(wqkv[l, 1, at], h[half:])
            value = value + column(ut, rows_q * t, rows_q, l)
            for n in range(heads):
                ref[n, 0:head, :] = value[n * head:(n + 1) * head].astype(BF16)

        def one_head(n, _):
            for start in range(0, cols, 256):
                at = pl.ds(start, 256)
                s = tn_dot(k3[n], q3[n, :, at])
                s = jnp.where(lax.broadcasted_iota(jnp.int32, s.shape, 0) < tokens, s, -1e30)
                e = jnp.exp2((s - jnp.max(s, axis=0, keepdims=True)) * factor)
                p = (e * (1.0 / jnp.sum(e, axis=0, keepdims=True))).astype(BF16)
                att[n, :, at] = nn_dot(v3[n], p)
            return 0
        lax.fori_loop(0, heads, one_head, 0)

        @pl.when(i == 0)
        def _():
            w_wait(l, (3,))
        packed = jnp.concatenate([att[n] for n in range(heads)], axis=0).astype(BF16)
        hid[0:rows_q, :] = packed
        project(l, i, lambda hf: tn_dot(wo[l, hf], hid[0:rows_q, :]))

    def mlp(l, i):
        @pl.when(i == 0)
        def _():
            w_wait(l, (4,))
        norm(i, 2 * l + 1)
        units = wup.shape[2]
        for a in range(0, units, 384):
            b = min(units, a + 384)
            u = tn_dot(wup[l, :, a:b], h[...]) + column(ut, a, b - a, 2 + l)
            hid[a:b, :] = gelu(u).astype(BF16)

        @pl.when(i == 0)
        def _():
            w_wait(l, (5,))
        project(l, i, lambda hf: nn_dot(wdn[l, pl.ds(pl.multiple_of(half * hf, 16), half)], hid[...]))

    for i in range(images):
        mine_in(i).start()
    for n in range(6):
        w_local(0, n).start()
    vec_own = pltpu.make_async_copy(vec_hbm, vraw.at[y, pl.ds(0, 16)], vec_sem.at[0])
    vec_own.start()
    col_own = pltpu.make_async_copy(col_hbm, uraw.at[pl.ds(0, 8)], col_sem)
    col_own.start()
    vec_row = send(vec_hbm, vraw.at[y, pl.ds(0, 16)], vec_sem.at[1], vec_sem.at[2], row)
    pl.semaphore_wait(barrier, 3)
    entry_row(0).start()
    vec_row.start()
    for n in range(3):
        w_remote(0, n).start()
    entry_row(1).start()
    entry_row(2).start()
    for n in range(3, 6):
        w_remote(0, n).start()
    for n in range(6):
        w_local(1, n).start()

    vraw[:, 16:, :] = jnp.zeros((2, vraw.shape[1] - 16, vraw.shape[2]), F32)
    uraw[8:, :] = jnp.zeros((uraw.shape[0] - 8, uraw.shape[1]), F32)
    q3[:, head:, :] = jnp.zeros((heads, q3.shape[1] - head, cols), BF16)
    k3[:, head:, :] = jnp.zeros((heads, k3.shape[1] - head, cols), BF16)
    col_own.wait()
    ut[...] = uraw[...].T
    vec_own.wait()
    vec_row.wait()
    for n in range(2):
        vt[n * half:(n + 1) * half, :] = vraw[n].T[:half]
    entry(0)

    def layer(l, _):
        def attn_step(i, _):
            k = 2 * images * l + i

            @pl.when(l == 0)
            def _():
                entry_done(i)

            @pl.when(l > 0)
            def _():
                gather_done(k)
            attend(l, i)
            stage_b(k)

            @pl.when(k == 0)
            def _():
                for j in range(1, images):
                    entry(j)
                for n in range(6):
                    w_remote(1, n).start()

            @pl.when(k >= 1)
            def _():
                stage_c(k - 1)

            @pl.when(k >= 2)
            def _():
                stage_d(k - 2)
            return 0
        lax.fori_loop(0, images, attn_step, 0)

        def mlp_step(i, _):
            k = 2 * images * l + images + i
            gather_done(k)
            mlp(l, i)
            stage_b(k)
            stage_c(k - 1)
            stage_d(k - 2)
            return 0
        lax.fori_loop(0, images, mlp_step, 0)
        return 0
    lax.fori_loop(0, 2, layer, 0)
    last = 4 * images - 1
    stage_c(last)
    stage_d(last - 1)
    stage_d(last)

    @pl.when(c == y)
    def _():
        for i in range(images):
            exit_local(i).wait()
            for kind in (1, 2, 3, 4, 5, 6):
                exit_copy(kind, i).wait_send()

    @pl.when(c != y)
    def _():
        for i in range(images):
            exit_copy(0, i).wait_send()
            for kind, own_row, at_x in ((2, True, x), (4, False, x), (5, True, 1 - x), (6, False, 1 - x)):
                piece = out_piece(own_row, i, at_x)
                send(piece, piece, ex_s.at[kind, i], ex_r.at[kind, i], sib).wait_recv()
    for l in range(2):
        for n in range(6):
            w_remote(l, n).wait_send()


def solution(mesh):
    act_spec = P("dp", None, "tx")
    vec_tx = P(None, "tx")
    proj_spec = P(None, "tx", "ty", None)
    head_vec = P(None, "ty", None)
    in_specs = (act_spec, vec_tx, vec_tx, proj_spec, head_vec, proj_spec, proj_spec, head_vec,
                P(None, "ty", None, "tx"), vec_tx, vec_tx, vec_tx,
                P(None, "tx", "ty"), P(None, "ty"), P(None, "ty", "tx"), vec_tx)

    def local_fn(x_in, ln1_gain, ln1_bias, w_q, b_q, w_k, w_v, b_v, w_o, b_o, ln2_gain, ln2_bias, w_up, b_up, w_down, b_down):
        total, tokens, half = x_in.shape
        layers, _, heads, head = w_q.shape
        units = w_up.shape[2]
        images, width, rows_q = total // 2, 2 * half, heads * head
        cols = -(-tokens // 256) * 256
        lanes = -(-half // 128) * 128
        long = -(-units // 128) * 128
        flat = lambda w: w.reshape(layers, half, rows_q).transpose(0, 2, 1)
        x_t = jnp.pad(x_in.transpose(0, 2, 1), ((0, 0), (0, 0), (0, cols - tokens)))
        pairs = ((ln1_gain, ln2_gain), (ln1_bias, ln2_bias), (b_o, b_down))
        vec = jnp.concatenate([v[l:l + 1] for a, b in pairs for l in range(layers) for v in (a, b)], axis=0)
        vec = jnp.pad(vec, ((0, 4), (0, lanes - half)))
        qkv_b = jnp.concatenate([b_q.reshape(layers, -1), jnp.zeros((layers, rows_q), F32), b_v.reshape(layers, -1)], axis=1)
        col = jnp.concatenate([jnp.pad(qkv_b, ((0, 0), (0, long - 3 * rows_q))), jnp.pad(b_up, ((0, 0), (0, long - units)))], axis=0)
        col = jnp.pad(col, ((0, 4), (0, 0)))
        dma = pltpu.SemaphoreType.DMA
        vmem = pltpu.VMEM
        y_t = pl.pallas_call(
            functools.partial(kernel, tokens),
            out_shape=jax.ShapeDtypeStruct((total, half, cols), BF16),
            in_specs=[pl.BlockSpec(memory_space=pl.ANY)] * 9,
            out_specs=pl.BlockSpec(memory_space=pl.ANY),
            scratch_shapes=[
                vmem((images, width, cols), BF16), vmem((width, cols), BF16), vmem((width, cols), BF16),
                vmem((images, half, cols), BF16), vmem((images, half // 2, cols), BF16),
                vmem((images, half // 2, cols), BF16), vmem((images, half // 2, cols), F32),
                vmem((heads, 128, cols), BF16), vmem((heads, 128, cols), BF16), vmem((heads, head, cols), BF16),
                vmem((heads, head, cols), F32), vmem((units, cols), BF16),
                vmem((layers, 2, 3 * rows_q, half), BF16), vmem((layers, 2, rows_q, half), BF16),
                vmem((layers, width, units), BF16), vmem((layers, width, units), BF16),
                vmem((2, 128, lanes), F32), vmem((128, long), F32), vmem((width, 128), F32), vmem((long, 128), F32),
                dma((2, 6)), dma((2, 6)), dma((2, 6)), dma((3,)), dma, dma((images,)),
                dma((4, images)), dma((4, images)), dma((images,)), dma((images,)),
                dma((images,)), dma((images,)), dma((3, images)), dma((3, images)),
                dma((7, images)), dma((7, images)),
            ],
            compiler_params=pltpu.CompilerParams(collective_id=0, has_side_effects=True, vmem_limit_bytes=66_000_000),
            name="encoder",
        )(x_t, vec, col, flat(w_q), flat(w_k), flat(w_v), w_o.reshape(layers, rows_q, half), w_up, w_down.transpose(0, 2, 1))
        return y_t[:, :, :tokens].transpose(0, 2, 1)

    return jax.shard_map(local_fn, mesh=mesh, in_specs=in_specs, out_specs=act_spec, check_vma=False)
```

```python
import jax
import jax.numpy as jnp
from jax import lax
from jax.experimental import pallas as pl
from jax.experimental.pallas import tpu as pltpu
from jax.sharding import PartitionSpec as P

EPS = 1e-6
MESH = pl.DeviceIdType.MESH
F32, BF16 = jnp.float32, jnp.bfloat16


def tn_dot(a, b):
    return lax.dot_general(a, b, (((0,), (0,)), ((), ())), preferred_element_type=F32)


def nn_dot(a, b):
    return jnp.dot(a, b, preferred_element_type=F32)


def gelu(u):
    return 0.5 * u * (1.0 + jnp.tanh(0.7978845608028654 * (u + 0.044715 * u * u * u)))


def kernel(x_hbm, g1_hbm, g2_hbm, s1_hbm, s2_hbm, bo_hbm, bd_hbm, bq_hbm, bv_hbm, bup_hbm, wq_hbm, wk_hbm, wv_hbm, wo_hbm, wup_hbm, wdn_hbm, out_hbm,
           xg, h, part, rd, rs, rr, acc, q3, k3, v3, att, hid, wqkv, wo, wup, wdn, vraw, craw, uraw, vpad, cpad, upad, vt, ct, ut,
           loc_sem, ws_sem, wr_sem, vec_sem, vec_s, vec_r, x_sem, en_s, en_r, d2_s, d2_r, rs_s, rs_r, ag_s, ag_r, ex_s, ex_r):
    dp, y, ty = lax.axis_index("dp"), lax.axis_index("tx"), lax.axis_index("ty")
    c, x = ty % 2, ty // 2
    images, width, tokens = xg.shape
    cols = h.shape[1]
    half, quarter, eighth = width // 2, width // 4, width // 8
    rows_q = 3 * wq_hbm.shape[1] // 3
    head = v3.shape[1]
    heads = v3.shape[0]
    sib = (dp, y, ty + 1 - 2 * c)
    across = (dp, y, (ty + 2) % 4)
    row = (dp, 1 - y, ty)

    barrier = pltpu.get_barrier_semaphore()
    for peer in (sib, across, row):
        pl.semaphore_signal(barrier, inc=1, device_id=peer, device_id_type=MESH)

    def send(src, dst, ssem, rsem, peer):
        return pltpu.make_async_remote_copy(src_ref=src, dst_ref=dst, send_sem=ssem, recv_sem=rsem,
                                            device_id=peer, device_id_type=MESH)

    def pieces(l):
        res = []
        for t, w in enumerate((wq_hbm, wk_hbm, wv_hbm)):
            res.append((w.at[l], wqkv.at[l, y, pl.ds(rows_q * t, rows_q)]))
        res.append((wo_hbm.at[l], wo.at[l, y]))
        res.append((wup_hbm.at[l], wup.at[l, pl.ds(half * y, half)]))
        res.append((wdn_hbm.at[l], wdn.at[l, pl.ds(half * y, half)]))
        return res

    def w_local(l, n):
        src, dst = pieces(l)[n]
        return pltpu.make_async_copy(src, dst, loc_sem.at[l, n])

    def w_remote(l, n):
        src, dst = pieces(l)[n]
        return send(src, dst, ws_sem.at[l, n], wr_sem.at[l, n], row)

    def w_wait(l, ns):
        for n in ns:
            w_local(l, n).wait()
            w_remote(l, n).wait_recv()

    def mine_in(i):
        return pltpu.make_async_copy(x_hbm.at[y * images + i], xg.at[i, pl.ds(half * y, half)], x_sem.at[i])

    def entry_row(i):
        at = eighth * (2 * c + x)
        return send(x_hbm.at[(1 - y) * images + i, pl.ds(at, eighth)],
                    xg.at[i, pl.ds(half * y + at, eighth)], en_s.at[0, i], en_r.at[0, i], row)

    def entry_fwd(kind, i):
        src_x = x if kind < 3 else 1 - x
        ref = xg.at[i, pl.ds(half * (1 - y) + eighth * (2 * c + src_x), eighth)]
        return send(ref, ref, en_s.at[kind, i], en_r.at[kind, i], across if kind == 1 else sib)

    def entry(i):
        entry_row(i).wait_recv()
        entry_fwd(1, i).start()
        entry_fwd(2, i).start()
        entry_fwd(1, i).wait_recv()
        entry_fwd(3, i).start()

    def entry_done(i):
        mine_in(i).wait()
        entry_fwd(2, i).wait_recv()
        entry_fwd(3, i).wait_recv()
        entry_row(i).wait_send()
        for kind in (1, 2, 3):
            entry_fwd(kind, i).wait_send()

    def d2d(i):
        return send(part.at[pl.ds(half * (1 - c), half)], rd.at[i], d2_s.at[i], d2_r.at[i], sib)

    def scatter(i):
        return send(rs.at[i], rr.at[i], rs_s.at[i], rs_r.at[i], across)

    def gather(kind, i):
        src_x = x if kind < 2 else 1 - x
        ref = xg.at[i, pl.ds(half * c + quarter * src_x, quarter)]
        return send(ref, ref, ag_s.at[kind, i], ag_r.at[kind, i], across if kind == 0 else sib)

    def stage_b(k):
        i = k % images
        d2d(i).wait_recv()
        mine, theirs = quarter * x, quarter * (1 - x)
        acc[i] = (part[pl.ds(pl.multiple_of(half * c + mine, 16), quarter)].astype(F32)
                  + rd[i, pl.ds(pl.multiple_of(mine, 16), quarter)].astype(F32))
        rs[i] = (part[pl.ds(pl.multiple_of(half * c + theirs, 16), quarter)].astype(F32)
                 + rd[i, pl.ds(pl.multiple_of(theirs, 16), quarter)].astype(F32)).astype(BF16)
        scatter(i).start()
        d2d(i).wait_send()

    def column(ref, at, size, lane):
        block = ref[pl.ds(at, size), :]
        picked = jnp.where(lax.broadcasted_iota(jnp.int32, block.shape, 1) == lane, block, 0.0)
        return jnp.sum(picked, axis=1, keepdims=True)

    def out_piece(own_row, i, at_x):
        image = (y if own_row else 1 - y) * images + i
        return out_hbm.at[image, pl.ds(quarter * at_x, quarter)]

    def final_piece(i):
        return xg.at[i, pl.ds(half * c + quarter * x, quarter)]

    def exit_copy(kind, i):
        sems = (ex_s.at[kind, i], ex_r.at[kind, i])
        if kind == 0:
            return send(final_piece(i), out_piece(True, i, x), *sems, row)
        if kind in (1, 2):
            return send(final_piece(i), out_piece(True, i, x), *sems, across if kind == 1 else sib)
        if kind in (3, 4):
            ref = out_piece(False, i, x)
            return send(ref, ref, *sems, across if kind == 3 else sib)
        ref = out_piece(kind == 5, i, 1 - x)
        return send(ref, ref, *sems, sib)

    def exit_local(i):
        return pltpu.make_async_copy(final_piece(i), out_piece(True, i, x), x_sem.at[i])

    def stage_c(k):
        i, s = k % images, k // images
        scatter(i).wait_recv()
        at = pl.multiple_of(half * c + quarter * x, 16)
        bias = column(vt, at, quarter, 8 + s)
        new = xg[i, pl.ds(at, quarter)].astype(F32) + (acc[i] + rr[i].astype(F32))[:, :tokens] + bias
        xg[i, pl.ds(at, quarter)] = new.astype(BF16)
        scatter(i).wait_send()

        @pl.when(s < 3)
        def _():
            gather(0, i).start()
            gather(1, i).start()

        @pl.when((s == 3) & (c == y))
        def _():
            exit_copy(1, i).start()
            exit_copy(2, i).start()
            exit_local(i).start()

        @pl.when((s == 3) & (c != y))
        def _():
            exit_copy(0, i).start()

    def stage_d(k):
        i, s = k % images, k // images

        @pl.when(s < 3)
        def _():
            gather(0, i).wait_recv()
            gather(2, i).start()

        @pl.when((s == 3) & (c == y))
        def _():
            send(final_piece(i), out_piece(False, i, x), ex_s.at[0, i], ex_r.at[0, i], row).wait_recv()
            exit_copy(3, i).start()
            exit_copy(4, i).start()
            send(final_piece(i), out_piece(True, i, 1 - x), ex_s.at[1, i], ex_r.at[1, i], across).wait_recv()
            exit_copy(5, i).start()
            piece = out_piece(False, i, 1 - x)
            send(piece, piece, ex_s.at[3, i], ex_r.at[3, i], across).wait_recv()
            exit_copy(6, i).start()

    def gather_done(k):
        i = k % images
        gather(1, i).wait_recv()
        gather(2, i).wait_recv()
        for kind in (0, 1, 2):
            gather(kind, i).wait_send()

    def norm(i, s):
        blocks = [pl.ds(b * quarter, quarter) for b in range(4)]
        total = sum(jnp.sum(xg[i, b].astype(F32), axis=0, keepdims=True) for b in blocks)
        mean = total / width
        spread = jnp.zeros_like(mean)
        for b in blocks:
            d = xg[i, b].astype(F32) - mean
            spread = spread + jnp.sum(d * d, axis=0, keepdims=True)
        inv = lax.rsqrt(spread / width + EPS)
        for n, b in enumerate(blocks):
            gain, shift = column(vt, n * quarter, quarter, s), column(vt, n * quarter, quarter, 4 + s)
            h[b, 0:tokens] = ((xg[i, b].astype(F32) - mean) * inv * gain + shift).astype(BF16)

    def project(l, i, make):
        def body(n, _):
            hf = (1 - c) * (1 - n) + c * n
            part[pl.ds(pl.multiple_of(half * hf, 16), half)] = make(hf).astype(BF16)

            @pl.when(n == 0)
            def _():
                d2d(i).start()
            return 0
        lax.fori_loop(0, 2, body, 0)

    factor = (head ** -0.5) * 1.4426950408889634

    def attend(l, i):
        @pl.when(i == 0)
        def _():
            w_wait(l, (0, 1, 2))
        norm(i, 2 * l)
        for t, ref in enumerate((q3, k3, v3)):
            at = pl.ds(rows_q * t, rows_q)
            value = nn_dot(wqkv[l, 0, at], h[:half]) + nn_dot(wqkv[l, 1, at], h[half:])
            for n in range(heads):
                one = value[n * head:(n + 1) * head]
                if t != 1:
                    one = one + column(ct, 0, head, heads * (t + l) + n)
                ref[n, 0:head, :] = one.astype(BF16)

        def one_head(n, _):
            for start in range(0, cols, 256):
                at = pl.ds(start, 256)
                s = tn_dot(k3[n], q3[n, :, at])
                s = jnp.where(lax.broadcasted_iota(jnp.int32, s.shape, 0) < tokens, s, -1e30)
                e = jnp.exp2((s - jnp.max(s, axis=0, keepdims=True)) * factor)
                p = (e * (1.0 / jnp.sum(e, axis=0, keepdims=True))).astype(BF16)
                att[n, :, at] = nn_dot(v3[n], p)
            return 0
        lax.fori_loop(0, heads, one_head, 0)

        @pl.when(i == 0)
        def _():
            w_wait(l, (3,))
        packed = jnp.concatenate([att[n] for n in range(heads)], axis=0).astype(BF16)
        hid[0:rows_q, :] = packed
        project(l, i, lambda hf: tn_dot(wo[l, hf], hid[0:rows_q, :]))

    def mlp(l, i):
        @pl.when(i == 0)
        def _():
            w_wait(l, (4,))
        norm(i, 2 * l + 1)
        units = wup.shape[2]
        for a in range(0, units, 384):
            b = min(units, a + 384)
            u = tn_dot(wup[l, :, a:b], h[...]) + column(ut, a, b - a, l)
            hid[a:b, :] = gelu(u).astype(BF16)

        @pl.when(i == 0)
        def _():
            w_wait(l, (5,))
        project(l, i, lambda hf: nn_dot(wdn[l, pl.ds(pl.multiple_of(half * hf, 16), half)], hid[...]))

    for i in range(images):
        mine_in(i).start()
    for n in range(6):
        w_local(0, n).start()
    vecs = (g1_hbm, g2_hbm, s1_hbm, s2_hbm, bo_hbm, bd_hbm)
    small = [pltpu.make_async_copy(v, vraw.at[y, n], vec_sem.at[n]) for n, v in enumerate(vecs)]
    small += [pltpu.make_async_copy(b, craw.at[n], vec_sem.at[6 + n]) for n, b in enumerate((bq_hbm, bv_hbm))]
    small.append(pltpu.make_async_copy(bup_hbm, uraw, vec_sem.at[8]))
    for copy in small:
        copy.start()
    vec_row = [send(v, vraw.at[y, n], vec_s.at[n], vec_r.at[n], row) for n, v in enumerate(vecs)]
    pl.semaphore_wait(barrier, 3)
    entry_row(0).start()
    for copy in vec_row:
        copy.start()
    for n in range(4):
        w_remote(0, n).start()
    for i in range(1, images):
        entry_row(i).start()
    for n in range(4, 6):
        w_remote(0, n).start()
    for n in range(6):
        w_local(1, n).start()

    layers = wup.shape[0]
    for ref in (vpad, cpad, upad):
        ref[...] = jnp.zeros_like(ref)
    h[:, cols - 128:] = jnp.zeros((width, 128), BF16)
    q3[:, head:, :] = jnp.zeros((heads, q3.shape[1] - head, cols), BF16)
    k3[:, head:, :] = jnp.zeros((heads, k3.shape[1] - head, cols), BF16)
    for copy in small:
        copy.wait()
    for l in range(layers):
        upad[l:l + 1, 0:uraw.shape[1]] = uraw[l:l + 1, :]
        for t in range(2):
            at = (2 * t + l) * heads
            cpad[at:at + heads, 0:head] = craw[t, l]
    ct[...] = cpad[...].T
    ut[...] = upad[...].T
    for copy in vec_row:
        copy.wait()
    for n in range(2):
        for a in range(6):
            for l in range(layers):
                at = 4 * (a // 2) + 2 * l + a % 2
                vpad[n, at:at + 1, 0:half] = vraw[n, a, l:l + 1, :]
        vt[n * half:(n + 1) * half, :] = vpad[n].T[:half]
    entry(0)

    def layer(l, _):
        def attn_step(i, _):
            k = 2 * images * l + i

            @pl.when(l == 0)
            def _():
                entry_done(i)

            @pl.when(l > 0)
            def _():
                gather_done(k)
            attend(l, i)
            stage_b(k)

            @pl.when(k == 0)
            def _():
                for j in range(1, images):
                    entry(j)
                for n in range(6):
                    w_remote(1, n).start()

            @pl.when(k >= 1)
            def _():
                stage_c(k - 1)

            @pl.when(k >= 2)
            def _():
                stage_d(k - 2)
            return 0
        lax.fori_loop(0, images, attn_step, 0)

        def mlp_step(i, _):
            k = 2 * images * l + images + i
            early = k == images

            @pl.when(early)
            def _():
                stage_c(k - 1)
                stage_d(k - 2)
                stage_d(k - 1)
            gather_done(k)
            mlp(l, i)
            stage_b(k)

            @pl.when(jnp.logical_not(early))
            def _():
                stage_c(k - 1)

            @pl.when((k != images) & (k != images + 1))
            def _():
                stage_d(k - 2)
            return 0
        lax.fori_loop(0, images, mlp_step, 0)
        return 0
    lax.fori_loop(0, 2, layer, 0)
    last = 4 * images - 1
    stage_c(last)
    stage_d(last - 1)
    stage_d(last)

    @pl.when(c == y)
    def _():
        for i in range(images):
            exit_local(i).wait()
            for kind in (1, 2, 3, 4, 5, 6):
                exit_copy(kind, i).wait_send()

    @pl.when(c != y)
    def _():
        for i in range(images):
            exit_copy(0, i).wait_send()
            for kind, own_row, at_x in ((2, True, x), (4, False, x), (5, True, 1 - x), (6, False, 1 - x)):
                piece = out_piece(own_row, i, at_x)
                send(piece, piece, ex_s.at[kind, i], ex_r.at[kind, i], sib).wait_recv()
    for l in range(2):
        for n in range(6):
            w_remote(l, n).wait_send()


def solution(mesh):
    act_spec = P("dp", None, "tx")
    vec_tx = P(None, "tx")
    proj_spec = P(None, "tx", "ty", None)
    head_vec = P(None, "ty", None)
    in_specs = (act_spec, vec_tx, vec_tx, proj_spec, head_vec, proj_spec, proj_spec, head_vec,
                P(None, "ty", None, "tx"), vec_tx, vec_tx, vec_tx,
                P(None, "tx", "ty"), P(None, "ty"), P(None, "ty", "tx"), vec_tx)

    def local_fn(x_in, ln1_gain, ln1_bias, w_q, b_q, w_k, w_v, b_v, w_o, b_o, ln2_gain, ln2_bias, w_up, b_up, w_down, b_down):
        total, tokens, half = x_in.shape
        layers, _, heads, head = w_q.shape
        units = w_up.shape[2]
        images, width, rows_q = total // 2, 2 * half, heads * head
        cols = -(-tokens // 256) * 256
        lanes = -(-half // 128) * 128
        long = -(-units // 128) * 128
        flat = lambda w: w.reshape(layers, half, rows_q).transpose(0, 2, 1)
        dma = pltpu.SemaphoreType.DMA
        vmem = pltpu.VMEM
        y_t = pl.pallas_call(
            kernel,
            out_shape=jax.ShapeDtypeStruct((total, half, tokens), BF16),
            in_specs=[pl.BlockSpec(memory_space=pl.ANY)] * 16,
            out_specs=pl.BlockSpec(memory_space=pl.ANY),
            scratch_shapes=[
                vmem((images, width, tokens), BF16), vmem((width, cols), BF16), vmem((width, cols), BF16),
                vmem((images, half, cols), BF16), vmem((images, half // 2, cols), BF16),
                vmem((images, half // 2, cols), BF16), vmem((images, half // 2, cols), F32),
                vmem((heads, 128, cols), BF16), vmem((heads, 128, cols), BF16), vmem((heads, head, cols), BF16),
                vmem((heads, head, cols), F32), vmem((units, cols), BF16),
                vmem((layers, 2, 3 * rows_q, half), BF16), vmem((layers, 2, rows_q, half), BF16),
                vmem((layers, width, units), BF16), vmem((layers, width, units), BF16),
                vmem((2, 6, layers, half), F32), vmem((2, layers, heads, head), F32), vmem((layers, units), F32),
                vmem((2, 128, lanes), F32), vmem((128, 128), F32), vmem((128, long), F32),
                vmem((width, 128), F32), vmem((128, 128), F32), vmem((long, 128), F32),
                dma((2, 6)), dma((2, 6)), dma((2, 6)), dma((9,)), dma((6,)), dma((6,)), dma((images,)),
                dma((4, images)), dma((4, images)), dma((images,)), dma((images,)),
                dma((images,)), dma((images,)), dma((3, images)), dma((3, images)),
                dma((7, images)), dma((7, images)),
            ],
            compiler_params=pltpu.CompilerParams(collective_id=0, has_side_effects=True, vmem_limit_bytes=66_000_000),
            name="encoder",
        )(x_in.transpose(0, 2, 1), ln1_gain, ln2_gain, ln1_bias, ln2_bias, b_o, b_down, b_q, b_v, b_up,
          flat(w_q), flat(w_k), flat(w_v), w_o.reshape(layers, rows_q, half), w_up, w_down.transpose(0, 2, 1))
        return y_t.transpose(0, 2, 1)

    return jax.shard_map(local_fn, mesh=mesh, in_specs=in_specs, out_specs=act_spec, check_vma=False)
```

```python
import jax
import jax.numpy as jnp
from jax import lax
from jax.experimental import pallas as pl
from jax.experimental.pallas import tpu as pltpu
from jax.sharding import PartitionSpec as P

EPS = 1e-6
MESH = pl.DeviceIdType.MESH
F32, BF16 = jnp.float32, jnp.bfloat16


def tn_dot(a, b):
    return lax.dot_general(a, b, (((0,), (0,)), ((), ())), preferred_element_type=F32)


def nn_dot(a, b):
    return jnp.dot(a, b, preferred_element_type=F32)


def gelu(u):
    return 0.5 * u * (1.0 + jnp.tanh(0.7978845608028654 * (u + 0.044715 * u * u * u)))


def kernel(x_hbm, g1_hbm, g2_hbm, s1_hbm, s2_hbm, bo_hbm, bd_hbm, bq_hbm, bv_hbm, bup_hbm, wq_hbm, wk_hbm, wv_hbm, wo_hbm, wup_hbm, wdn_hbm, out_hbm,
           xg, h, part, rd, rs, rr, acc, q3, k3, v3, att, hid, wqkv, wo, wup, wdn, vraw, craw, uraw, vpad, cpad, upad, vt, ct, ut,
           loc_sem, ws_sem, wr_sem, vec_sem, vec_s, vec_r, x_sem, en_s, en_r, d2_s, d2_r, rs_s, rs_r, ag_s, ag_r, ex_s, ex_r):
    dp, y, ty = lax.axis_index("dp"), lax.axis_index("tx"), lax.axis_index("ty")
    c, x = ty % 2, ty // 2
    images, width, tokens = xg.shape
    cols = h.shape[1]
    half, quarter, eighth = width // 2, width // 4, width // 8
    rows_q = 3 * wq_hbm.shape[1] // 3
    head = v3.shape[1]
    heads = v3.shape[0]
    sib = (dp, y, ty + 1 - 2 * c)
    across = (dp, y, (ty + 2) % 4)
    row = (dp, 1 - y, ty)

    barrier = pltpu.get_barrier_semaphore()
    for peer in (sib, across, row):
        pl.semaphore_signal(barrier, inc=1, device_id=peer, device_id_type=MESH)

    def send(src, dst, ssem, rsem, peer):
        return pltpu.make_async_remote_copy(src_ref=src, dst_ref=dst, send_sem=ssem, recv_sem=rsem,
                                            device_id=peer, device_id_type=MESH)

    def pieces(l):
        res = []
        for t, w in enumerate((wq_hbm, wk_hbm, wv_hbm)):
            res.append((w.at[l], wqkv.at[l, y, pl.ds(rows_q * t, rows_q)]))
        res.append((wo_hbm.at[l], wo.at[l, y]))
        res.append((wup_hbm.at[l], wup.at[l, pl.ds(half * y, half)]))
        res.append((wdn_hbm.at[l], wdn.at[l, pl.ds(half * y, half)]))
        return res

    def w_local(l, n):
        src, dst = pieces(l)[n]
        return pltpu.make_async_copy(src, dst, loc_sem.at[l, n])

    def w_remote(l, n):
        src, dst = pieces(l)[n]
        return send(src, dst, ws_sem.at[l, n], wr_sem.at[l, n], row)

    def w_wait(l, ns):
        for n in ns:
            w_local(l, n).wait()
            w_remote(l, n).wait_recv()

    def mine_in(i):
        return pltpu.make_async_copy(x_hbm.at[y * images + i], xg.at[i, pl.ds(half * y, half)], x_sem.at[i])

    def entry_row(i):
        at = eighth * (2 * c + x)
        return send(x_hbm.at[(1 - y) * images + i, pl.ds(at, eighth)],
                    xg.at[i, pl.ds(half * y + at, eighth)], en_s.at[0, i], en_r.at[0, i], row)

    def entry_fwd(kind, i):
        src_x = x if kind < 3 else 1 - x
        ref = xg.at[i, pl.ds(half * (1 - y) + eighth * (2 * c + src_x), eighth)]
        return send(ref, ref, en_s.at[kind, i], en_r.at[kind, i], across if kind == 1 else sib)

    def entry(i):
        entry_row(i).wait_recv()
        entry_fwd(1, i).start()
        entry_fwd(2, i).start()
        entry_fwd(1, i).wait_recv()
        entry_fwd(3, i).start()

    def entry_done(i):
        mine_in(i).wait()
        entry_fwd(2, i).wait_recv()
        entry_fwd(3, i).wait_recv()
        entry_row(i).wait_send()
        for kind in (1, 2, 3):
            entry_fwd(kind, i).wait_send()

    def d2d(i):
        return send(part.at[pl.ds(half * (1 - c), half)], rd.at[i], d2_s.at[i], d2_r.at[i], sib)

    def scatter(i):
        return send(rs.at[i], rr.at[i], rs_s.at[i], rs_r.at[i], across)

    def gather(kind, i):
        src_x = x if kind < 2 else 1 - x
        ref = xg.at[i, pl.ds(half * c + quarter * src_x, quarter)]
        return send(ref, ref, ag_s.at[kind, i], ag_r.at[kind, i], across if kind == 0 else sib)

    def stage_b(k):
        i = k % images
        d2d(i).wait_recv()
        mine, theirs = quarter * x, quarter * (1 - x)
        acc[i] = (part[pl.ds(pl.multiple_of(half * c + mine, 16), quarter)].astype(F32)
                  + rd[i, pl.ds(pl.multiple_of(mine, 16), quarter)].astype(F32))
        rs[i] = (part[pl.ds(pl.multiple_of(half * c + theirs, 16), quarter)].astype(F32)
                 + rd[i, pl.ds(pl.multiple_of(theirs, 16), quarter)].astype(F32)).astype(BF16)
        scatter(i).start()
        d2d(i).wait_send()

    def column(ref, at, size, lane):
        block = ref[pl.ds(at, size), :]
        picked = jnp.where(lax.broadcasted_iota(jnp.int32, block.shape, 1) == lane, block, 0.0)
        return jnp.sum(picked, axis=1, keepdims=True)

    def out_piece(own_row, i, at_x):
        image = (y if own_row else 1 - y) * images + i
        return out_hbm.at[image, pl.ds(quarter * at_x, quarter)]

    def final_piece(i):
        return xg.at[i, pl.ds(half * c + quarter * x, quarter)]

    def exit_copy(kind, i):
        sems = (ex_s.at[kind, i], ex_r.at[kind, i])
        if kind == 0:
            return send(final_piece(i), out_piece(True, i, x), *sems, row)
        if kind in (1, 2):
            return send(final_piece(i), out_piece(True, i, x), *sems, across if kind == 1 else sib)
        if kind in (3, 4):
            ref = out_piece(False, i, x)
            return send(ref, ref, *sems, across if kind == 3 else sib)
        ref = out_piece(kind == 5, i, 1 - x)
        return send(ref, ref, *sems, sib)

    def exit_local(i):
        return pltpu.make_async_copy(final_piece(i), out_piece(True, i, x), x_sem.at[i])

    def stage_c(k):
        i, s = k % images, k // images
        scatter(i).wait_recv()
        at = pl.multiple_of(half * c + quarter * x, 16)
        bias = column(vt, at, quarter, 8 + s)
        new = xg[i, pl.ds(at, quarter)].astype(F32) + (acc[i] + rr[i].astype(F32))[:, :tokens] + bias
        xg[i, pl.ds(at, quarter)] = new.astype(BF16)
        scatter(i).wait_send()

        @pl.when(s < 3)
        def _():
            gather(0, i).start()
            gather(1, i).start()

        @pl.when((s == 3) & (c == y))
        def _():
            exit_copy(1, i).start()
            exit_copy(2, i).start()
            exit_local(i).start()

        @pl.when((s == 3) & (c != y))
        def _():
            exit_copy(0, i).start()

    def stage_d(k):
        i, s = k % images, k // images

        @pl.when(s < 3)
        def _():
            gather(0, i).wait_recv()
            gather(2, i).start()

        @pl.when((s == 3) & (c == y))
        def _():
            send(final_piece(i), out_piece(False, i, x), ex_s.at[0, i], ex_r.at[0, i], row).wait_recv()
            exit_copy(3, i).start()
            exit_copy(4, i).start()
            send(final_piece(i), out_piece(True, i, 1 - x), ex_s.at[1, i], ex_r.at[1, i], across).wait_recv()
            exit_copy(5, i).start()
            piece = out_piece(False, i, 1 - x)
            send(piece, piece, ex_s.at[3, i], ex_r.at[3, i], across).wait_recv()
            exit_copy(6, i).start()

    def gather_done(k):
        i = k % images
        gather(1, i).wait_recv()
        gather(2, i).wait_recv()
        for kind in (0, 1, 2):
            gather(kind, i).wait_send()

    def norm(i, s):
        blocks = [pl.ds(b * quarter, quarter) for b in range(4)]
        total = sum(jnp.sum(xg[i, b].astype(F32), axis=0, keepdims=True) for b in blocks)
        mean = total / width
        spread = jnp.zeros_like(mean)
        for b in blocks:
            d = xg[i, b].astype(F32) - mean
            spread = spread + jnp.sum(d * d, axis=0, keepdims=True)
        inv = lax.rsqrt(spread / width + EPS)
        for n, b in enumerate(blocks):
            gain, shift = column(vt, n * quarter, quarter, s), column(vt, n * quarter, quarter, 4 + s)
            h[b, 0:tokens] = ((xg[i, b].astype(F32) - mean) * inv * gain + shift).astype(BF16)

    def project(l, i, make):
        def body(n, _):
            hf = (1 - c) * (1 - n) + c * n
            part[pl.ds(pl.multiple_of(half * hf, 16), half)] = make(hf).astype(BF16)

            @pl.when(n == 0)
            def _():
                d2d(i).start()
            return 0
        lax.fori_loop(0, 2, body, 0)

    factor = (head ** -0.5) * 1.4426950408889634

    def attend(l, i):
        norm(i, 2 * l)
        for t, ref in enumerate((q3, k3, v3)):
            @pl.when(i == 0)
            def _():
                w_wait(l, (t,))
            at = pl.ds(rows_q * t, rows_q)
            value = nn_dot(wqkv[l, 0, at], h[:half]) + nn_dot(wqkv[l, 1, at], h[half:])
            for n in range(heads):
                one = value[n * head:(n + 1) * head]
                if t != 1:
                    one = one + column(ct, 0, head, heads * (t + l) + n)
                ref[n, 0:head, :] = one.astype(BF16)

        edge, top = -(-tokens // 16) * 16, tokens // 16 * 16

        def one_head(n, _):
            s = nn_dot(k3[n].T[:edge], q3[n])
            tail = s[top:]
            tail = jnp.where(lax.broadcasted_iota(jnp.int32, tail.shape, 0) + top < tokens, tail, -1e30)
            s = jnp.concatenate([s[:top], tail], axis=0)
            e = jnp.exp2((s - jnp.max(s, axis=0, keepdims=True)) * factor)
            p = (e * (1.0 / jnp.sum(e, axis=0, keepdims=True))).astype(BF16)
            att[n] = nn_dot(v3[n, :, :edge], p)
            return 0
        lax.fori_loop(0, heads, one_head, 0, unroll=2)

        @pl.when(i == 0)
        def _():
            w_wait(l, (3,))
        packed = jnp.concatenate([att[n] for n in range(heads)], axis=0).astype(BF16)
        hid[0:rows_q, :] = packed
        project(l, i, lambda hf: tn_dot(wo[l, hf], hid[0:rows_q, :]))

    def mlp(l, i):
        norm(i, 2 * l + 1)

        @pl.when(i == 0)
        def _():
            w_wait(l, (4,))
        units = wup.shape[2]
        for a in range(0, units, 384):
            b = min(units, a + 384)
            u = tn_dot(wup[l, :, a:b], h[...]) + column(ut, a, b - a, l)
            hid[a:b, :] = gelu(u).astype(BF16)

        @pl.when(i == 0)
        def _():
            w_wait(l, (5,))
        project(l, i, lambda hf: nn_dot(wdn[l, pl.ds(pl.multiple_of(half * hf, 16), half)], hid[...]))

    for i in range(images):
        mine_in(i).start()
    for n in range(6):
        w_local(0, n).start()
    vecs = (g1_hbm, g2_hbm, s1_hbm, s2_hbm, bo_hbm, bd_hbm)
    small = [pltpu.make_async_copy(v, vraw.at[y, n], vec_sem.at[n]) for n, v in enumerate(vecs)]
    small += [pltpu.make_async_copy(b, craw.at[n], vec_sem.at[6 + n]) for n, b in enumerate((bq_hbm, bv_hbm))]
    small.append(pltpu.make_async_copy(bup_hbm, uraw, vec_sem.at[8]))
    for copy in small:
        copy.start()
    vec_row = [send(v, vraw.at[y, n], vec_s.at[n], vec_r.at[n], row) for n, v in enumerate(vecs)]
    pl.semaphore_wait(barrier, 3)
    entry_row(0).start()
    for copy in vec_row:
        copy.start()
    for n in range(4):
        w_remote(0, n).start()
    for i in range(1, images):
        entry_row(i).start()
    for n in range(4, 6):
        w_remote(0, n).start()
    for n in range(6):
        w_local(1, n).start()

    layers = wup.shape[0]
    for ref in (vpad, cpad, upad):
        ref[...] = jnp.zeros_like(ref)
    h[:, cols - 128:] = jnp.zeros((width, 128), BF16)
    q3[:, head:, :] = jnp.zeros((heads, q3.shape[1] - head, cols), BF16)
    k3[:, head:, :] = jnp.zeros((heads, k3.shape[1] - head, cols), BF16)
    for copy in small:
        copy.wait()
    for l in range(layers):
        upad[l:l + 1, 0:uraw.shape[1]] = uraw[l:l + 1, :]
        for t in range(2):
            at = (2 * t + l) * heads
            cpad[at:at + heads, 0:head] = craw[t, l]
    ct[...] = cpad[...].T
    ut[...] = upad[...].T
    for copy in vec_row:
        copy.wait()
    for n in range(2):
        for a in range(6):
            for l in range(layers):
                at = 4 * (a // 2) + 2 * l + a % 2
                vpad[n, at:at + 1, 0:half] = vraw[n, a, l:l + 1, :]
        vt[n * half:(n + 1) * half, :] = vpad[n].T[:half]
    entry(0)

    def layer(l, _):
        def attn_step(i, _):
            k = 2 * images * l + i

            @pl.when(l == 0)
            def _():
                entry_done(i)

            @pl.when(l > 0)
            def _():
                gather_done(k)
            attend(l, i)
            stage_b(k)

            @pl.when(k == 0)
            def _():
                for j in range(1, images):
                    entry(j)
                for n in range(6):
                    w_remote(1, n).start()

            @pl.when(k >= 1)
            def _():
                stage_c(k - 1)

            @pl.when(k >= 2)
            def _():
                stage_d(k - 2)
            return 0
        lax.fori_loop(0, images, attn_step, 0)

        def mlp_step(i, _):
            k = 2 * images * l + images + i
            early = k == images

            @pl.when(early)
            def _():
                stage_c(k - 1)
                stage_d(k - 2)
            gather_done(k)
            mlp(l, i)
            stage_b(k)

            @pl.when(jnp.logical_not(early))
            def _():
                stage_c(k - 1)

            @pl.when(jnp.logical_not(early))
            def _():
                stage_d(k - 2)
            return 0
        lax.fori_loop(0, images, mlp_step, 0)
        return 0
    lax.fori_loop(0, 2, layer, 0)
    last = 4 * images - 1
    stage_c(last)
    stage_d(last - 1)
    stage_d(last)

    @pl.when(c == y)
    def _():
        for i in range(images):
            exit_local(i).wait()
            for kind in (1, 2, 3, 4, 5, 6):
                exit_copy(kind, i).wait_send()

    @pl.when(c != y)
    def _():
        for i in range(images):
            exit_copy(0, i).wait_send()
            for kind, own_row, at_x in ((2, True, x), (4, False, x), (5, True, 1 - x), (6, False, 1 - x)):
                piece = out_piece(own_row, i, at_x)
                send(piece, piece, ex_s.at[kind, i], ex_r.at[kind, i], sib).wait_recv()
    for l in range(2):
        for n in range(6):
            w_remote(l, n).wait_send()


def solution(mesh):
    act_spec = P("dp", None, "tx")
    vec_tx = P(None, "tx")
    proj_spec = P(None, "tx", "ty", None)
    head_vec = P(None, "ty", None)
    in_specs = (act_spec, vec_tx, vec_tx, proj_spec, head_vec, proj_spec, proj_spec, head_vec,
                P(None, "ty", None, "tx"), vec_tx, vec_tx, vec_tx,
                P(None, "tx", "ty"), P(None, "ty"), P(None, "ty", "tx"), vec_tx)

    def local_fn(x_in, ln1_gain, ln1_bias, w_q, b_q, w_k, w_v, b_v, w_o, b_o, ln2_gain, ln2_bias, w_up, b_up, w_down, b_down):
        total, tokens, half = x_in.shape
        layers, _, heads, head = w_q.shape
        units = w_up.shape[2]
        images, width, rows_q = total // 2, 2 * half, heads * head
        cols = -(-tokens // 256) * 256
        lanes = -(-half // 128) * 128
        long = -(-units // 128) * 128
        flat = lambda w: w.reshape(layers, half, rows_q).transpose(0, 2, 1)
        dma = pltpu.SemaphoreType.DMA
        vmem = pltpu.VMEM
        y_t = pl.pallas_call(
            kernel,
            out_shape=jax.ShapeDtypeStruct((total, half, tokens), BF16),
            in_specs=[pl.BlockSpec(memory_space=pl.ANY)] * 16,
            out_specs=pl.BlockSpec(memory_space=pl.ANY),
            scratch_shapes=[
                vmem((images, width, tokens), BF16), vmem((width, cols), BF16), vmem((width, cols), BF16),
                vmem((images, half, cols), BF16), vmem((images, half // 2, cols), BF16),
                vmem((images, half // 2, cols), BF16), vmem((images, half // 2, cols), F32),
                vmem((heads, 128, cols), BF16), vmem((heads, 128, cols), BF16), vmem((heads, head, cols), BF16),
                vmem((heads, head, cols), F32), vmem((units, cols), BF16),
                vmem((layers, 2, 3 * rows_q, half), BF16), vmem((layers, 2, rows_q, half), BF16),
                vmem((layers, width, units), BF16), vmem((layers, width, units), BF16),
                vmem((2, 6, layers, half), F32), vmem((2, layers, heads, head), F32), vmem((layers, units), F32),
                vmem((2, 128, lanes), F32), vmem((128, 128), F32), vmem((128, long), F32),
                vmem((width, 128), F32), vmem((128, 128), F32), vmem((long, 128), F32),
                dma((2, 6)), dma((2, 6)), dma((2, 6)), dma((9,)), dma((6,)), dma((6,)), dma((images,)),
                dma((4, images)), dma((4, images)), dma((images,)), dma((images,)),
                dma((images,)), dma((images,)), dma((3, images)), dma((3, images)),
                dma((7, images)), dma((7, images)),
            ],
            compiler_params=pltpu.CompilerParams(collective_id=0, has_side_effects=True, vmem_limit_bytes=66_000_000),
            name="encoder",
        )(x_in.transpose(0, 2, 1), ln1_gain, ln2_gain, ln1_bias, ln2_bias, b_o, b_down, b_q, b_v, b_up,
          flat(w_q), flat(w_k), flat(w_v), w_o.reshape(layers, rows_q, half), w_up, w_down.transpose(0, 2, 1))
        return y_t.transpose(0, 2, 1)

    return jax.shard_map(local_fn, mesh=mesh, in_specs=in_specs, out_specs=act_spec, check_vma=False)
```

```python
import jax
import jax.numpy as jnp
from jax import lax
from jax.experimental import pallas as pl
from jax.experimental.pallas import tpu as pltpu
from jax.sharding import PartitionSpec as P

EPS = 1e-6
MESH = pl.DeviceIdType.MESH
F32, BF16 = jnp.float32, jnp.bfloat16
CUTS = 3


def tn_dot(a, b):
    return lax.dot_general(a, b, (((0,), (0,)), ((), ())), preferred_element_type=F32)


def nn_dot(a, b):
    return jnp.dot(a, b, preferred_element_type=F32)


def gelu(u):
    return 0.5 * u * (1.0 + jnp.tanh(0.7978845608028654 * (u + 0.044715 * u * u * u)))


def kernel(x_hbm, g1_hbm, g2_hbm, s1_hbm, s2_hbm, bo_hbm, bd_hbm, bq_hbm, bv_hbm, bup_hbm, wq_hbm, wk_hbm, wv_hbm, wo_hbm, wup_hbm, wdn_hbm, out_hbm,
           xg, h, part, rd, rs, rr, acc, q3, k3, v3, att, hid, wqkv, wo, wup, wdn, vraw, craw, uraw, vpad, cpad, upad, vt, ct, ut,
           loc_sem, ws_sem, wr_sem, vec_sem, vec_s, vec_r, x_sem, en_s, en_r, d2_s, d2_r, rs_s, rs_r, ag_s, ag_r, ex_s, ex_r, lo_sem):
    dp, y, ty = lax.axis_index("dp"), lax.axis_index("tx"), lax.axis_index("ty")
    c, x = ty % 2, ty // 2
    images, width, tokens = xg.shape
    cols = h.shape[1]
    half, quarter, eighth = width // 2, width // 4, width // 8
    rows_q = 3 * wq_hbm.shape[1] // 3
    head = v3.shape[1]
    heads = v3.shape[0]
    sib = (dp, y, ty + 1 - 2 * c)
    across = (dp, y, (ty + 2) % 4)
    row = (dp, 1 - y, ty)

    barrier = pltpu.get_barrier_semaphore()
    for peer in (sib, across, row):
        pl.semaphore_signal(barrier, inc=1, device_id=peer, device_id_type=MESH)

    def send(src, dst, ssem, rsem, peer):
        return pltpu.make_async_remote_copy(src_ref=src, dst_ref=dst, send_sem=ssem, recv_sem=rsem,
                                            device_id=peer, device_id_type=MESH)

    def pieces(l):
        res = []
        for t, w in enumerate((wq_hbm, wk_hbm, wv_hbm)):
            res.append((w.at[l], wqkv.at[l, y, pl.ds(rows_q * t, rows_q)]))
        res.append((wo_hbm.at[l], wo.at[l, y]))
        res.append((wup_hbm.at[l], wup.at[l, pl.ds(half * y, half)]))
        res.append((wdn_hbm.at[l], wdn.at[l, pl.ds(half * y, half)]))
        return res

    def w_local(l, n):
        src, dst = pieces(l)[n]
        return pltpu.make_async_copy(src, dst, loc_sem.at[l, n])

    def w_remote(l, n):
        src, dst = pieces(l)[n]
        return send(src, dst, ws_sem.at[l, n], wr_sem.at[l, n], row)

    def w_wait(l, ns):
        for n in ns:
            w_local(l, n).wait()
            w_remote(l, n).wait_recv()

    def mine_in(i):
        return pltpu.make_async_copy(x_hbm.at[y * images + i], xg.at[i, pl.ds(half * y, half)], x_sem.at[i])

    def entry_row(i):
        at = eighth * (2 * c + x)
        return send(x_hbm.at[(1 - y) * images + i, pl.ds(at, eighth)],
                    xg.at[i, pl.ds(half * y + at, eighth)], en_s.at[0, i], en_r.at[0, i], row)

    def entry_fwd(kind, i):
        src_x = x if kind < 3 else 1 - x
        ref = xg.at[i, pl.ds(half * (1 - y) + eighth * (2 * c + src_x), eighth)]
        return send(ref, ref, en_s.at[kind, i], en_r.at[kind, i], across if kind == 1 else sib)

    def entry(i):
        entry_row(i).wait_recv()
        entry_fwd(1, i).start()
        entry_fwd(2, i).start()
        entry_fwd(1, i).wait_recv()
        entry_fwd(3, i).start()

    def entry_done(i):
        mine_in(i).wait()
        entry_fwd(2, i).wait_recv()
        entry_fwd(3, i).wait_recv()
        entry_row(i).wait_send()
        for kind in (1, 2, 3):
            entry_fwd(kind, i).wait_send()

    def d2d(i):
        return send(part.at[pl.ds(half * (1 - c), half)], rd.at[i], d2_s.at[i], d2_r.at[i], sib)

    cut = quarter // CUTS

    def scatter(i, j):
        at = pl.ds(cut * j, cut)
        return send(rs.at[i, at], rr.at[i, at], rs_s.at[i, j], rs_r.at[i, j], across)

    def gather(kind, i):
        src_x = x if kind < 2 else 1 - x
        ref = xg.at[i, pl.ds(half * c + quarter * src_x, quarter)]
        return send(ref, ref, ag_s.at[kind, i], ag_r.at[kind, i], across if kind == 0 else sib)

    def stage_b(k):
        i = k % images
        d2d(i).wait_recv()
        mine, theirs = quarter * x, quarter * (1 - x)
        acc[i] = (part[pl.ds(pl.multiple_of(half * c + mine, 16), quarter)].astype(F32)
                  + rd[i, pl.ds(pl.multiple_of(mine, 16), quarter)].astype(F32))
        rs[i] = (part[pl.ds(pl.multiple_of(half * c + theirs, 16), quarter)].astype(F32)
                 + rd[i, pl.ds(pl.multiple_of(theirs, 16), quarter)].astype(F32)).astype(BF16)
        for j in range(CUTS):
            scatter(i, j).start()
        d2d(i).wait_send()

    def column(ref, at, size, lane):
        block = ref[pl.ds(at, size), :]
        picked = jnp.where(lax.broadcasted_iota(jnp.int32, block.shape, 1) == lane, block, 0.0)
        return jnp.sum(picked, axis=1, keepdims=True)

    def out_piece(own_row, i, j, at_x):
        image = (y if own_row else 1 - y) * images + i
        return out_hbm.at[image, pl.ds(quarter * at_x + cut * j, cut)]

    def final_piece(i, j):
        return xg.at[i, pl.ds(half * c + quarter * x + cut * j, cut)]

    def exit_copy(kind, i, j):
        sems = (ex_s.at[kind, i, j], ex_r.at[kind, i, j])
        if kind == 0:
            return send(final_piece(i, j), out_piece(True, i, j, x), *sems, row)
        if kind in (1, 2):
            return send(final_piece(i, j), out_piece(True, i, j, x), *sems, across if kind == 1 else sib)
        if kind in (3, 4):
            ref = out_piece(False, i, j, x)
            return send(ref, ref, *sems, across if kind == 3 else sib)
        ref = out_piece(kind == 5, i, j, 1 - x)
        return send(ref, ref, *sems, sib)

    def exit_local(i, j):
        return pltpu.make_async_copy(final_piece(i, j), out_piece(True, i, j, x), lo_sem.at[i, j])

    def stage_c(k):
        i, s = k % images, k // images
        for j in range(CUTS):
            scatter(i, j).wait_recv()
            at = pl.multiple_of(half * c + quarter * x + cut * j, 16)
            bias = column(vt, at, cut, 8 + s)
            got = acc[i, cut * j:cut * (j + 1)] + rr[i, cut * j:cut * (j + 1)].astype(F32)
            new = xg[i, pl.ds(at, cut)].astype(F32) + got[:, :tokens] + bias
            xg[i, pl.ds(at, cut)] = new.astype(BF16)

            @pl.when((s == 3) & (c == y))
            def _():
                exit_copy(1, i, j).start()
                exit_copy(2, i, j).start()
                exit_local(i, j).start()

            @pl.when((s == 3) & (c != y))
            def _():
                exit_copy(0, i, j).start()

        for j in range(CUTS):
            scatter(i, j).wait_send()

        @pl.when(s < 3)
        def _():
            gather(0, i).start()
            gather(1, i).start()

    def exit_row(i):
        @pl.when(c == y)
        def _():
            for j in range(CUTS):
                send(final_piece(i, j), out_piece(False, i, j, x), ex_s.at[0, i, j], ex_r.at[0, i, j], row).wait_recv()
                exit_copy(3, i, j).start()
                exit_copy(4, i, j).start()

    def exit_across(i):
        @pl.when(c == y)
        def _():
            for own_row, kind in ((True, 1), (False, 3)):
                for j in range(CUTS):
                    piece = out_piece(own_row, i, j, 1 - x)
                    send(piece, piece, ex_s.at[kind, i, j], ex_r.at[kind, i, j], across).wait_recv()
                    exit_copy(5 if own_row else 6, i, j).start()

    def stage_d(k):
        i, s = k % images, k // images

        @pl.when(s < 3)
        def _():
            gather(0, i).wait_recv()
            gather(2, i).start()

        @pl.when(s == 3)
        def _():
            exit_row(i)
            exit_across(i)

    def gather_done(k):
        i = k % images
        gather(1, i).wait_recv()
        gather(2, i).wait_recv()
        for kind in (0, 1, 2):
            gather(kind, i).wait_send()

    def norm(i, s):
        blocks = [pl.ds(b * quarter, quarter) for b in range(4)]
        total = sum(jnp.sum(xg[i, b].astype(F32), axis=0, keepdims=True) for b in blocks)
        mean = total / width
        spread = jnp.zeros_like(mean)
        for b in blocks:
            d = xg[i, b].astype(F32) - mean
            spread = spread + jnp.sum(d * d, axis=0, keepdims=True)
        inv = lax.rsqrt(spread / width + EPS)
        for n, b in enumerate(blocks):
            gain, shift = column(vt, n * quarter, quarter, s), column(vt, n * quarter, quarter, 4 + s)
            h[b, 0:tokens] = ((xg[i, b].astype(F32) - mean) * inv * gain + shift).astype(BF16)

    def project(l, i, make):
        def body(n, _):
            hf = (1 - c) * (1 - n) + c * n
            part[pl.ds(pl.multiple_of(half * hf, 16), half)] = make(hf).astype(BF16)

            @pl.when(n == 0)
            def _():
                d2d(i).start()
            return 0
        lax.fori_loop(0, 2, body, 0)

    factor = (head ** -0.5) * 1.4426950408889634

    def attend(l, i):
        norm(i, 2 * l)
        for t, ref in enumerate((q3, k3, v3)):
            @pl.when(i == 0)
            def _():
                w_wait(l, (t,))
            at = pl.ds(rows_q * t, rows_q)
            value = nn_dot(wqkv[l, 0, at], h[:half]) + nn_dot(wqkv[l, 1, at], h[half:])
            for n in range(heads):
                one = value[n * head:(n + 1) * head]
                if t != 1:
                    one = one + column(ct, 0, head, heads * (t + l) + n)
                ref[n, 0:head, :] = one.astype(BF16)

        edge, top = -(-tokens // 16) * 16, tokens // 16 * 16

        def one_head(n, _):
            s = nn_dot(k3[n].T[:edge], q3[n])
            tail = s[top:]
            tail = jnp.where(lax.broadcasted_iota(jnp.int32, tail.shape, 0) + top < tokens, tail, -1e30)
            s = jnp.concatenate([s[:top], tail], axis=0)
            e = jnp.exp2((s - jnp.max(s, axis=0, keepdims=True)) * factor)
            p = (e * (1.0 / jnp.sum(e, axis=0, keepdims=True))).astype(BF16)
            att[n] = nn_dot(v3[n, :, :edge], p)
            return 0
        lax.fori_loop(0, heads, one_head, 0, unroll=2)

        @pl.when(i == 0)
        def _():
            w_wait(l, (3,))
        packed = jnp.concatenate([att[n] for n in range(heads)], axis=0).astype(BF16)
        hid[0:rows_q, :] = packed
        project(l, i, lambda hf: tn_dot(wo[l, hf], hid[0:rows_q, :]))

    def mlp(l, i):
        norm(i, 2 * l + 1)

        @pl.when(i == 0)
        def _():
            w_wait(l, (4,))
        units = wup.shape[2]
        for a in range(0, units, 384):
            b = min(units, a + 384)
            u = tn_dot(wup[l, :, a:b], h[...]) + column(ut, a, b - a, l)
            hid[a:b, :] = gelu(u).astype(BF16)

        @pl.when(i == 0)
        def _():
            w_wait(l, (5,))
        project(l, i, lambda hf: nn_dot(wdn[l, pl.ds(pl.multiple_of(half * hf, 16), half)], hid[...]))

    for i in range(images):
        mine_in(i).start()
    for n in range(6):
        w_local(0, n).start()
    vecs = (g1_hbm, g2_hbm, s1_hbm, s2_hbm, bo_hbm, bd_hbm)
    small = [pltpu.make_async_copy(v, vraw.at[y, n], vec_sem.at[n]) for n, v in enumerate(vecs)]
    small += [pltpu.make_async_copy(b, craw.at[n], vec_sem.at[6 + n]) for n, b in enumerate((bq_hbm, bv_hbm))]
    small.append(pltpu.make_async_copy(bup_hbm, uraw, vec_sem.at[8]))
    for copy in small:
        copy.start()
    vec_row = [send(v, vraw.at[y, n], vec_s.at[n], vec_r.at[n], row) for n, v in enumerate(vecs)]
    pl.semaphore_wait(barrier, 3)
    entry_row(0).start()
    for copy in vec_row:
        copy.start()
    for n in range(4):
        w_remote(0, n).start()
    for i in range(1, images):
        entry_row(i).start()
    for n in range(4, 6):
        w_remote(0, n).start()
    for n in range(6):
        w_local(1, n).start()

    layers = wup.shape[0]
    for ref in (vpad, cpad, upad):
        ref[...] = jnp.zeros_like(ref)
    h[:, cols - 128:] = jnp.zeros((width, 128), BF16)
    q3[:, head:, :] = jnp.zeros((heads, q3.shape[1] - head, cols), BF16)
    k3[:, head:, :] = jnp.zeros((heads, k3.shape[1] - head, cols), BF16)
    for copy in small:
        copy.wait()
    for l in range(layers):
        upad[l:l + 1, 0:uraw.shape[1]] = uraw[l:l + 1, :]
        for t in range(2):
            at = (2 * t + l) * heads
            cpad[at:at + heads, 0:head] = craw[t, l]
    ct[...] = cpad[...].T
    ut[...] = upad[...].T
    for copy in vec_row:
        copy.wait()
    for n in range(2):
        for a in range(6):
            for l in range(layers):
                at = 4 * (a // 2) + 2 * l + a % 2
                vpad[n, at:at + 1, 0:half] = vraw[n, a, l:l + 1, :]
        vt[n * half:(n + 1) * half, :] = vpad[n].T[:half]
    entry(0)

    def layer(l, _):
        def attn_step(i, _):
            k = 2 * images * l + i

            @pl.when(l == 0)
            def _():
                entry_done(i)

            @pl.when(l > 0)
            def _():
                gather_done(k)
            attend(l, i)
            stage_b(k)

            @pl.when(k == 0)
            def _():
                for j in range(1, images):
                    entry(j)
                for n in range(6):
                    w_remote(1, n).start()

            @pl.when(k >= 1)
            def _():
                stage_c(k - 1)

            @pl.when(k >= 2)
            def _():
                stage_d(k - 2)
            return 0
        lax.fori_loop(0, images, attn_step, 0)

        def mlp_step(i, _):
            k = 2 * images * l + images + i
            early = k == images

            @pl.when(early)
            def _():
                stage_c(k - 1)
                stage_d(k - 2)
            gather_done(k)
            mlp(l, i)
            stage_b(k)

            @pl.when(jnp.logical_not(early))
            def _():
                stage_c(k - 1)

            @pl.when(jnp.logical_not(early))
            def _():
                stage_d(k - 2)
            return 0
        lax.fori_loop(0, images, mlp_step, 0)
        return 0
    lax.fori_loop(0, 2, layer, 0)
    last = images - 1
    exit_row(last - 1)
    stage_c(4 * images - 1)
    exit_across(last - 1)
    exit_row(last)
    exit_across(last)

    @pl.when(c == y)
    def _():
        for i in range(images):
            for j in range(CUTS):
                exit_local(i, j).wait()
                for kind in (1, 2, 3, 4, 5, 6):
                    exit_copy(kind, i, j).wait_send()

    @pl.when(c != y)
    def _():
        for i in range(images):
            for j in range(CUTS):
                exit_copy(0, i, j).wait_send()
                for kind, own_row, at_x in ((2, True, x), (4, False, x), (5, True, 1 - x), (6, False, 1 - x)):
                    piece = out_piece(own_row, i, j, at_x)
                    send(piece, piece, ex_s.at[kind, i, j], ex_r.at[kind, i, j], sib).wait_recv()
    for l in range(2):
        for n in range(6):
            w_remote(l, n).wait_send()


def solution(mesh):
    act_spec = P("dp", None, "tx")
    vec_tx = P(None, "tx")
    proj_spec = P(None, "tx", "ty", None)
    head_vec = P(None, "ty", None)
    in_specs = (act_spec, vec_tx, vec_tx, proj_spec, head_vec, proj_spec, proj_spec, head_vec,
                P(None, "ty", None, "tx"), vec_tx, vec_tx, vec_tx,
                P(None, "tx", "ty"), P(None, "ty"), P(None, "ty", "tx"), vec_tx)

    def local_fn(x_in, ln1_gain, ln1_bias, w_q, b_q, w_k, w_v, b_v, w_o, b_o, ln2_gain, ln2_bias, w_up, b_up, w_down, b_down):
        total, tokens, half = x_in.shape
        layers, _, heads, head = w_q.shape
        units = w_up.shape[2]
        images, width, rows_q = total // 2, 2 * half, heads * head
        cols = -(-tokens // 256) * 256
        lanes = -(-half // 128) * 128
        long = -(-units // 128) * 128
        flat = lambda w: w.reshape(layers, half, rows_q).transpose(0, 2, 1)
        dma = pltpu.SemaphoreType.DMA
        vmem = pltpu.VMEM
        y_t = pl.pallas_call(
            kernel,
            out_shape=jax.ShapeDtypeStruct((total, half, tokens), BF16),
            in_specs=[pl.BlockSpec(memory_space=pl.ANY)] * 16,
            out_specs=pl.BlockSpec(memory_space=pl.ANY),
            scratch_shapes=[
                vmem((images, width, tokens), BF16), vmem((width, cols), BF16), vmem((width, cols), BF16),
                vmem((images, half, cols), BF16), vmem((images, half // 2, cols), BF16),
                vmem((images, half // 2, cols), BF16), vmem((images, half // 2, cols), F32),
                vmem((heads, 128, cols), BF16), vmem((heads, 128, cols), BF16), vmem((heads, head, cols), BF16),
                vmem((heads, head, cols), F32), vmem((units, cols), BF16),
                vmem((layers, 2, 3 * rows_q, half), BF16), vmem((layers, 2, rows_q, half), BF16),
                vmem((layers, width, units), BF16), vmem((layers, width, units), BF16),
                vmem((2, 6, layers, half), F32), vmem((2, layers, heads, head), F32), vmem((layers, units), F32),
                vmem((2, 128, lanes), F32), vmem((128, 128), F32), vmem((128, long), F32),
                vmem((width, 128), F32), vmem((128, 128), F32), vmem((long, 128), F32),
                dma((2, 6)), dma((2, 6)), dma((2, 6)), dma((9,)), dma((6,)), dma((6,)), dma((images,)),
                dma((4, images)), dma((4, images)), dma((images,)), dma((images,)),
                dma((images, CUTS)), dma((images, CUTS)), dma((3, images)), dma((3, images)),
                dma((7, images, CUTS)), dma((7, images, CUTS)), dma((images, CUTS)),
            ],
            compiler_params=pltpu.CompilerParams(collective_id=0, has_side_effects=True, vmem_limit_bytes=66_000_000),
            name="encoder",
        )(x_in.transpose(0, 2, 1), ln1_gain, ln2_gain, ln1_bias, ln2_bias, b_o, b_down, b_q, b_v, b_up,
          flat(w_q), flat(w_k), flat(w_v), w_o.reshape(layers, rows_q, half), w_up, w_down.transpose(0, 2, 1))
        return y_t.transpose(0, 2, 1)

    return jax.shard_map(local_fn, mesh=mesh, in_specs=in_specs, out_specs=act_spec, check_vma=False)
```

```python
import jax
import jax.numpy as jnp
from jax import lax
from jax.experimental import pallas as pl
from jax.experimental.pallas import tpu as pltpu
from jax.sharding import PartitionSpec as P

EPS = 1e-6
MESH = pl.DeviceIdType.MESH
F32, BF16 = jnp.float32, jnp.bfloat16
CUTS = 3


def tn_dot(a, b):
    return lax.dot_general(a, b, (((0,), (0,)), ((), ())), preferred_element_type=F32)


def nn_dot(a, b):
    return jnp.dot(a, b, preferred_element_type=F32)


def gelu(u):
    return 0.5 * u * (1.0 + jnp.tanh(0.7978845608028654 * (u + 0.044715 * u * u * u)))


def kernel(x_hbm, g1_hbm, g2_hbm, s1_hbm, s2_hbm, bo_hbm, bd_hbm, bq_hbm, bv_hbm, bup_hbm, wq_hbm, wk_hbm, wv_hbm, wo_hbm, wup_hbm, wdn_hbm, out_hbm,
           xg, h, part, rd, rs, rr, acc, q3, k3, v3, att, every, hid, wqkv, wo, wup, wdn, vraw, craw, uraw, vpad, cpad, upad, vt, ct, ut,
           loc_sem, ws_sem, wr_sem, vec_sem, vec_s, vec_r, x_sem, en_s, en_r, d2_s, d2_r, rs_s, rs_r, ag_s, ag_r, ex_s, ex_r, lo_sem,
           at_s, at_r, hx_s, hx_r, wo_loc, wo_s, wo_r):
    dp, y, ty = lax.axis_index("dp"), lax.axis_index("tx"), lax.axis_index("ty")
    c, x = ty % 2, ty // 2
    images, width, tokens = xg.shape
    cols = h.shape[1]
    half, quarter, eighth = width // 2, width // 4, width // 8
    rows_q = 3 * wq_hbm.shape[1] // 3
    head = v3.shape[1]
    heads = v3.shape[0]
    sib = (dp, y, ty + 1 - 2 * c)
    across = (dp, y, (ty + 2) % 4)
    row = (dp, 1 - y, ty)

    barrier = pltpu.get_barrier_semaphore()
    for peer in (sib, across, row, (dp, y, 3 - ty), (dp, 1 - y, ty + 1 - 2 * c)):
        pl.semaphore_signal(barrier, inc=1, device_id=peer, device_id_type=MESH)

    def send(src, dst, ssem, rsem, peer):
        return pltpu.make_async_remote_copy(src_ref=src, dst_ref=dst, send_sem=ssem, recv_sem=rsem,
                                            device_id=peer, device_id_type=MESH)

    def pieces(l):
        res = []
        for t, w in enumerate((wq_hbm, wk_hbm, wv_hbm)):
            res.append((w.at[l], wqkv.at[l, y, pl.ds(rows_q * t, rows_q)]))
        res.append((wup_hbm.at[l], wup.at[l, pl.ds(half * y, half)]))
        res.append((wdn_hbm.at[l], wdn.at[l, pl.ds(half * y, half)]))
        return res

    def w_local(l, n):
        src, dst = pieces(l)[n]
        return pltpu.make_async_copy(src, dst, loc_sem.at[l, n])

    def w_remote(l, n):
        src, dst = pieces(l)[n]
        return send(src, dst, ws_sem.at[l, n], wr_sem.at[l, n], row)

    def w_wait(l, ns):
        for n in ns:
            w_local(l, n).wait()
            w_remote(l, n).wait_recv()

    def wo_send(l, kind):
        peer = ((dp, y, 2 * x + y), (dp, y, 2 * (1 - x) + y), (dp, 1 - y, 2 * x + y))[kind]
        return send(wo_hbm.at[l], wo.at[l, ty], wo_s.at[l, kind], wo_r.at[l, ty], peer)

    def wo_local(l):
        return pltpu.make_async_copy(wo_hbm.at[l], wo.at[l, ty], wo_loc.at[l])

    def wo_here(l):
        @pl.when(c == y)
        def _():
            wo_local(l).start()

        @pl.when(c != y)
        def _():
            wo_send(l, 0).start()

    def wo_pass(l, n):
        ref = wo.at[l, 2 * x + n]
        return send(ref, ref, wo_s.at[l, 3 + n], wo_r.at[l, 2 * x + n], across)

    def wo_came(l, block):
        send(wo_hbm.at[l], wo.at[l, block], wo_s.at[l, 0], wo_r.at[l, block], across).wait_recv()

    def wo_fwd(l):
        @pl.when(c != y)
        def _():
            for n in range(2):
                wo_came(l, 2 * x + n)
                wo_pass(l, n).start()

    def wo_wait(l):
        for n in range(2):
            wo_came(l, 2 * (1 - x) + n)

        @pl.when(c == y)
        def _():
            wo_local(l).wait()
            wo_came(l, ty + 1 - 2 * c)

    def wo_end(l):
        for kind in (1, 2):
            wo_send(l, kind).wait_send()

        @pl.when(c != y)
        def _():
            wo_send(l, 0).wait_send()
            for n in range(2):
                wo_pass(l, n).wait_send()

    def mine_in(i):
        return pltpu.make_async_copy(x_hbm.at[y * images + i], xg.at[i, pl.ds(half * y, half)], x_sem.at[i])

    def entry_row(i):
        at = eighth * (2 * c + x)
        return send(x_hbm.at[(1 - y) * images + i, pl.ds(at, eighth)],
                    xg.at[i, pl.ds(half * y + at, eighth)], en_s.at[0, i], en_r.at[0, i], row)

    def entry_fwd(kind, i):
        src_x = x if kind < 3 else 1 - x
        ref = xg.at[i, pl.ds(half * (1 - y) + eighth * (2 * c + src_x), eighth)]
        return send(ref, ref, en_s.at[kind, i], en_r.at[kind, i], across if kind == 1 else sib)

    def entry(i):
        entry_row(i).wait_recv()
        entry_fwd(1, i).start()
        entry_fwd(2, i).start()
        entry_fwd(1, i).wait_recv()
        entry_fwd(3, i).start()

    def entry_done(i):
        mine_in(i).wait()
        entry_fwd(2, i).wait_recv()
        entry_fwd(3, i).wait_recv()
        entry_row(i).wait_send()
        for kind in (1, 2, 3):
            entry_fwd(kind, i).wait_send()

    def d2d(i):
        return send(part.at[pl.ds(half * (1 - c), half)], rd.at[i], d2_s.at[i], d2_r.at[i], sib)

    cut = quarter // CUTS

    def scatter(i, j):
        at = pl.ds(cut * j, cut)
        return send(rs.at[i, at], rr.at[i, at], rs_s.at[i, j], rs_r.at[i, j], across)

    def gather(kind, i):
        src_x = x if kind < 2 else 1 - x
        ref = xg.at[i, pl.ds(half * c + quarter * src_x, quarter)]
        return send(ref, ref, ag_s.at[kind, i], ag_r.at[kind, i], across if kind == 0 else sib)

    def stage_b(k):
        i = k % images
        d2d(i).wait_recv()
        mine, theirs = quarter * x, quarter * (1 - x)
        acc[i] = (part[pl.ds(pl.multiple_of(half * c + mine, 16), quarter)].astype(F32)
                  + rd[i, pl.ds(pl.multiple_of(mine, 16), quarter)].astype(F32))
        rs[i] = (part[pl.ds(pl.multiple_of(half * c + theirs, 16), quarter)].astype(F32)
                 + rd[i, pl.ds(pl.multiple_of(theirs, 16), quarter)].astype(F32)).astype(BF16)
        for j in range(CUTS):
            scatter(i, j).start()
        d2d(i).wait_send()

    def column(ref, at, size, lane):
        block = ref[pl.ds(at, size), :]
        picked = jnp.where(lax.broadcasted_iota(jnp.int32, block.shape, 1) == lane, block, 0.0)
        return jnp.sum(picked, axis=1, keepdims=True)

    def out_piece(own_row, i, j, at_x):
        image = (y if own_row else 1 - y) * images + i
        return out_hbm.at[image, pl.ds(quarter * at_x + cut * j, cut)]

    def final_piece(i, j):
        return xg.at[i, pl.ds(half * c + quarter * x + cut * j, cut)]

    def exit_copy(kind, i, j):
        sems = (ex_s.at[kind, i, j], ex_r.at[kind, i, j])
        if kind == 0:
            return send(final_piece(i, j), out_piece(True, i, j, x), *sems, row)
        if kind in (1, 2):
            return send(final_piece(i, j), out_piece(True, i, j, x), *sems, across if kind == 1 else sib)
        if kind in (3, 4):
            ref = out_piece(False, i, j, x)
            return send(ref, ref, *sems, across if kind == 3 else sib)
        ref = out_piece(kind == 5, i, j, 1 - x)
        return send(ref, ref, *sems, sib)

    def exit_local(i, j):
        return pltpu.make_async_copy(final_piece(i, j), out_piece(True, i, j, x), lo_sem.at[i, j])

    def stage_c(k):
        i, s = k % images, k // images
        for j in range(CUTS):
            scatter(i, j).wait_recv()
            at = pl.multiple_of(half * c + quarter * x + cut * j, 16)
            bias = column(vt, at, cut, 8 + s)
            got = acc[i, cut * j:cut * (j + 1)] + rr[i, cut * j:cut * (j + 1)].astype(F32)
            new = xg[i, pl.ds(at, cut)].astype(F32) + got[:, :tokens] + bias
            xg[i, pl.ds(at, cut)] = new.astype(BF16)

            @pl.when((s == 3) & (c == y))
            def _():
                exit_copy(1, i, j).start()
                exit_copy(2, i, j).start()
                exit_local(i, j).start()

            @pl.when((s == 3) & (c != y))
            def _():
                exit_copy(0, i, j).start()

        for j in range(CUTS):
            scatter(i, j).wait_send()

        @pl.when(s < 3)
        def _():
            gather(0, i).start()
            gather(1, i).start()

    def exit_row(i):
        @pl.when(c == y)
        def _():
            for j in range(CUTS):
                send(final_piece(i, j), out_piece(False, i, j, x), ex_s.at[0, i, j], ex_r.at[0, i, j], row).wait_recv()
                exit_copy(3, i, j).start()
                exit_copy(4, i, j).start()

    def exit_across(i):
        @pl.when(c == y)
        def _():
            for own_row, kind in ((True, 1), (False, 3)):
                for j in range(CUTS):
                    piece = out_piece(own_row, i, j, 1 - x)
                    send(piece, piece, ex_s.at[kind, i, j], ex_r.at[kind, i, j], across).wait_recv()
                    exit_copy(5 if own_row else 6, i, j).start()

    def stage_d(k):
        i, s = k % images, k // images

        @pl.when(s < 3)
        def _():
            gather(0, i).wait_recv()
            gather(2, i).start()

        @pl.when(s == 3)
        def _():
            exit_row(i)
            exit_across(i)

    def gather_done(k):
        i = k % images
        gather(1, i).wait_recv()
        gather(2, i).wait_recv()
        for kind in (0, 1, 2):
            gather(kind, i).wait_send()

    def norm(i, s):
        blocks = [pl.ds(b * quarter, quarter) for b in range(4)]
        total = sum(jnp.sum(xg[i, b].astype(F32), axis=0, keepdims=True) for b in blocks)
        mean = total / width
        spread = jnp.zeros_like(mean)
        for b in blocks:
            d = xg[i, b].astype(F32) - mean
            spread = spread + jnp.sum(d * d, axis=0, keepdims=True)
        inv = lax.rsqrt(spread / width + EPS)
        for n, b in enumerate(blocks):
            gain, shift = column(vt, n * quarter, quarter, s), column(vt, n * quarter, quarter, 4 + s)
            h[b, 0:tokens] = ((xg[i, b].astype(F32) - mean) * inv * gain + shift).astype(BF16)

    def project(l, i, make):
        def body(n, _):
            hf = (1 - c) * (1 - n) + c * n
            part[pl.ds(pl.multiple_of(half * hf, 16), half)] = make(hf).astype(BF16)

            @pl.when(n == 0)
            def _():
                d2d(i).start()
            return 0
        lax.fori_loop(0, 2, body, 0)

    factor = (head ** -0.5) * 1.4426950408889634

    def attend(l, i):
        norm(i, 2 * l)
        for t, ref in enumerate((q3, k3, v3)):
            @pl.when(i == 0)
            def _():
                w_wait(l, (t,))
            at = pl.ds(rows_q * t, rows_q)
            value = nn_dot(wqkv[l, 0, at], h[:half]) + nn_dot(wqkv[l, 1, at], h[half:])
            for n in range(heads):
                one = value[n * head:(n + 1) * head]
                if t != 1:
                    one = one + column(ct, 0, head, heads * (t + l) + n)
                ref[n, 0:head, :] = one.astype(BF16)

        edge, top = -(-tokens // 16) * 16, tokens // 16 * 16

        def one_head(n, _):
            s = nn_dot(k3[n].T[:edge], q3[n])
            tail = s[top:]
            tail = jnp.where(lax.broadcasted_iota(jnp.int32, tail.shape, 0) + top < tokens, tail, -1e30)
            s = jnp.concatenate([s[:top], tail], axis=0)
            e = jnp.exp2((s - jnp.max(s, axis=0, keepdims=True)) * factor)
            p = (e * (1.0 / jnp.sum(e, axis=0, keepdims=True))).astype(BF16)
            att[n] = nn_dot(v3[n, :, :edge], p)
            return 0
        lax.fori_loop(0, heads, one_head, 0, unroll=2)

        packed = jnp.concatenate([att[n] for n in range(heads)], axis=0).astype(BF16)
        every[i, pl.ds(pl.multiple_of(rows_q * ty, 16), rows_q), :] = packed
        att_copy(0, i).start()
        att_copy(1, i).start()

    def att_copy(kind, i):
        owner = ty if kind < 2 else (ty + 2) % 4
        ref = every.at[i, pl.ds(rows_q * owner, rows_q)]
        return send(ref, ref, at_s.at[kind, i], at_r.at[kind, i], across if kind == 0 else sib)

    def half_copy(i):
        ref = xg.at[i, pl.ds(half * c, half)]
        return send(ref, ref, hx_s.at[i], hx_r.at[i], sib)

    def att_fwd(i):
        att_copy(0, i).wait_recv()
        att_copy(2, i).start()

    def att_out(l, i):
        @pl.when(i == 0)
        def _():
            wo_wait(l)
        att_copy(1, i).wait_recv()
        att_copy(2, i).wait_recv()
        at = pl.multiple_of(half * c, 16)
        value = tn_dot(wo[l].reshape(width, half), every[i]) + column(vt, at, half, 8 + 2 * l)
        xg[i, pl.ds(at, half)] = (xg[i, pl.ds(at, half)].astype(F32) + value[:, :tokens]).astype(BF16)
        half_copy(i).start()
        for kind in range(3):
            att_copy(kind, i).wait_send()

    def mlp(l, i):
        half_copy(i).wait_recv()
        half_copy(i).wait_send()
        norm(i, 2 * l + 1)

        @pl.when(i == 0)
        def _():
            w_wait(l, (3,))
        units = wup.shape[2]
        for a in range(0, units, 384):
            b = min(units, a + 384)
            u = tn_dot(wup[l, :, a:b], h[...]) + column(ut, a, b - a, l)
            hid[a:b, :] = gelu(u).astype(BF16)

        @pl.when(i == 0)
        def _():
            att_fwd(images - 1)
            att_out(l, images - 1)
            w_wait(l, (4,))
        project(l, i, lambda hf: nn_dot(wdn[l, pl.ds(pl.multiple_of(half * hf, 16), half)], hid[...]))

    for i in range(images):
        mine_in(i).start()
    for n in range(5):
        w_local(0, n).start()
    vecs = (g1_hbm, g2_hbm, s1_hbm, s2_hbm, bo_hbm, bd_hbm)
    small = [pltpu.make_async_copy(v, vraw.at[y, n], vec_sem.at[n]) for n, v in enumerate(vecs)]
    small += [pltpu.make_async_copy(b, craw.at[n], vec_sem.at[6 + n]) for n, b in enumerate((bq_hbm, bv_hbm))]
    small.append(pltpu.make_async_copy(bup_hbm, uraw, vec_sem.at[8]))
    for copy in small:
        copy.start()
    vec_row = [send(v, vraw.at[y, n], vec_s.at[n], vec_r.at[n], row) for n, v in enumerate(vecs)]
    pl.semaphore_wait(barrier, 5)
    entry_row(0).start()
    for copy in vec_row:
        copy.start()
    wo_here(0)
    wo_send(0, 1).start()
    for n in range(3):
        w_remote(0, n).start()
    wo_send(0, 2).start()
    for i in range(1, images):
        entry_row(i).start()
    for n in range(3, 5):
        w_remote(0, n).start()
    wo_here(1)
    wo_send(1, 1).start()
    for n in range(5):
        w_local(1, n).start()

    layers = wup.shape[0]
    for ref in (vpad, cpad, upad):
        ref[...] = jnp.zeros_like(ref)
    h[:, cols - 128:] = jnp.zeros((width, 128), BF16)
    q3[:, head:, :] = jnp.zeros((heads, q3.shape[1] - head, cols), BF16)
    k3[:, head:, :] = jnp.zeros((heads, k3.shape[1] - head, cols), BF16)
    for copy in small:
        copy.wait()
    for l in range(layers):
        upad[l:l + 1, 0:uraw.shape[1]] = uraw[l:l + 1, :]
        for t in range(2):
            at = (2 * t + l) * heads
            cpad[at:at + heads, 0:head] = craw[t, l]
    ct[...] = cpad[...].T
    ut[...] = upad[...].T
    for copy in vec_row:
        copy.wait()
    for n in range(2):
        for a in range(6):
            for l in range(layers):
                at = 4 * (a // 2) + 2 * l + a % 2
                vpad[n, at:at + 1, 0:half] = vraw[n, a, l:l + 1, :]
        vt[n * half:(n + 1) * half, :] = vpad[n].T[:half]
    entry(0)

    def layer(l, _):
        def attn_step(i, _):
            k = 2 * images * l + i

            @pl.when(l == 0)
            def _():
                entry_done(i)

            @pl.when(l > 0)
            def _():
                gather_done(k)
            attend(l, i)

            @pl.when(i >= 1)
            def _():
                att_fwd(i - 1)

            @pl.when((l > 0) & (i == 0))
            def _():
                stage_c(k - 1)

            @pl.when((l > 0) & (i <= 1))
            def _():
                stage_d(k - 2)

            @pl.when(i == 0)
            def _():
                wo_fwd(l)

            @pl.when(k == 0)
            def _():
                for j in range(1, images):
                    entry(j)
                for n in range(3):
                    w_remote(1, n).start()
                wo_send(1, 2).start()
                for n in range(3, 5):
                    w_remote(1, n).start()

            @pl.when(i >= 1)
            def _():
                att_out(l, i - 1)
            return 0
        lax.fori_loop(0, images, attn_step, 0)

        def mlp_step(i, _):
            k = 2 * images * l + images + i
            mlp(l, i)
            stage_b(k)

            @pl.when(i >= 1)
            def _():
                stage_c(k - 1)

            @pl.when(i >= 2)
            def _():
                stage_d(k - 2)
            return 0
        lax.fori_loop(0, images, mlp_step, 0)
        return 0
    lax.fori_loop(0, 2, layer, 0)
    last = images - 1
    exit_row(last - 1)
    stage_c(4 * images - 1)
    exit_across(last - 1)
    exit_row(last)
    exit_across(last)

    @pl.when(c == y)
    def _():
        for i in range(images):
            for j in range(CUTS):
                exit_local(i, j).wait()
                for kind in (1, 2, 3, 4, 5, 6):
                    exit_copy(kind, i, j).wait_send()

    @pl.when(c != y)
    def _():
        for i in range(images):
            for j in range(CUTS):
                exit_copy(0, i, j).wait_send()
                for kind, own_row, at_x in ((2, True, x), (4, False, x), (5, True, 1 - x), (6, False, 1 - x)):
                    piece = out_piece(own_row, i, j, at_x)
                    send(piece, piece, ex_s.at[kind, i, j], ex_r.at[kind, i, j], sib).wait_recv()
    for l in range(2):
        wo_end(l)
        for n in range(5):
            w_remote(l, n).wait_send()


def solution(mesh):
    act_spec = P("dp", None, "tx")
    vec_tx = P(None, "tx")
    proj_spec = P(None, "tx", "ty", None)
    head_vec = P(None, "ty", None)
    in_specs = (act_spec, vec_tx, vec_tx, proj_spec, head_vec, proj_spec, proj_spec, head_vec,
                P(None, "ty", None, "tx"), vec_tx, vec_tx, vec_tx,
                P(None, "tx", "ty"), P(None, "ty"), P(None, "ty", "tx"), vec_tx)

    def local_fn(x_in, ln1_gain, ln1_bias, w_q, b_q, w_k, w_v, b_v, w_o, b_o, ln2_gain, ln2_bias, w_up, b_up, w_down, b_down):
        total, tokens, half = x_in.shape
        layers, _, heads, head = w_q.shape
        units = w_up.shape[2]
        images, width, rows_q = total // 2, 2 * half, heads * head
        cols = -(-tokens // 256) * 256
        lanes = -(-half // 128) * 128
        long = -(-units // 128) * 128
        flat = lambda w: w.reshape(layers, half, rows_q).transpose(0, 2, 1)
        dma = pltpu.SemaphoreType.DMA
        vmem = pltpu.VMEM
        y_t = pl.pallas_call(
            kernel,
            out_shape=jax.ShapeDtypeStruct((total, half, tokens), BF16),
            in_specs=[pl.BlockSpec(memory_space=pl.ANY)] * 16,
            out_specs=pl.BlockSpec(memory_space=pl.ANY),
            scratch_shapes=[
                vmem((images, width, tokens), BF16), vmem((width, cols), BF16), vmem((width, cols), BF16),
                vmem((images, half, cols), BF16), vmem((images, half // 2, cols), BF16),
                vmem((images, half // 2, cols), BF16), vmem((images, half // 2, cols), F32),
                vmem((heads, 128, cols), BF16), vmem((heads, 128, cols), BF16), vmem((heads, head, cols), BF16),
                vmem((heads, head, cols), F32), vmem((images, width, cols), BF16), vmem((units, cols), BF16),
                vmem((layers, 2, 3 * rows_q, half), BF16), vmem((layers, 4, rows_q, half), BF16),
                vmem((layers, width, units), BF16), vmem((layers, width, units), BF16),
                vmem((2, 6, layers, half), F32), vmem((2, layers, heads, head), F32), vmem((layers, units), F32),
                vmem((2, 128, lanes), F32), vmem((128, 128), F32), vmem((128, long), F32),
                vmem((width, 128), F32), vmem((128, 128), F32), vmem((long, 128), F32),
                dma((2, 5)), dma((2, 5)), dma((2, 5)), dma((9,)), dma((6,)), dma((6,)), dma((images,)),
                dma((4, images)), dma((4, images)), dma((images,)), dma((images,)),
                dma((images, CUTS)), dma((images, CUTS)), dma((3, images)), dma((3, images)),
                dma((7, images, CUTS)), dma((7, images, CUTS)), dma((images, CUTS)),
                dma((3, images)), dma((3, images)), dma((images,)), dma((images,)), dma((2,)), dma((2, 5)), dma((2, 4)),
            ],
            compiler_params=pltpu.CompilerParams(collective_id=0, has_side_effects=True, vmem_limit_bytes=66_000_000),
            name="encoder",
        )(x_in.transpose(0, 2, 1), ln1_gain, ln2_gain, ln1_bias, ln2_bias, b_o, b_down, b_q, b_v, b_up,
          flat(w_q), flat(w_k), flat(w_v), w_o.reshape(layers, rows_q, half), w_up, w_down.transpose(0, 2, 1))
        return y_t.transpose(0, 2, 1)

    return jax.shard_map(local_fn, mesh=mesh, in_specs=in_specs, out_specs=act_spec, check_vma=False)
```

```python
import jax
import jax.numpy as jnp
from jax import lax
from jax.experimental import pallas as pl
from jax.experimental.pallas import tpu as pltpu
from jax.sharding import PartitionSpec as P

EPS = 1e-6
MESH = pl.DeviceIdType.MESH
F32, BF16 = jnp.float32, jnp.bfloat16
CUTS = 3


def tn_dot(a, b):
    return lax.dot_general(a, b, (((0,), (0,)), ((), ())), preferred_element_type=F32)


def nn_dot(a, b):
    return jnp.dot(a, b, preferred_element_type=F32)


def gelu(u):
    return 0.5 * u * (1.0 + jnp.tanh(0.7978845608028654 * (u + 0.044715 * u * u * u)))


def kernel(x_hbm, g1_hbm, g2_hbm, s1_hbm, s2_hbm, bo_hbm, bd_hbm, bq_hbm, bv_hbm, bup_hbm, wq_hbm, wk_hbm, wv_hbm, wo_hbm, wup_hbm, wdn_hbm, out_hbm,
           xg, h, part, rd, rs, rr, acc, q3, k3, v3, att, every, wqkv, wo, wup, wdn, vraw, craw, uraw, vpad, cpad, upad, vt, ct, ut,
           loc_sem, ws_sem, wr_sem, vec_sem, vec_s, vec_r, x_sem, en_s, en_r, d2_s, d2_r, rs_s, rs_r, ag_s, ag_r, ex_s, ex_r, lo_sem,
           at_s, at_r, hx_s, hx_r, wo_loc, wo_s, wo_r):
    dp, y, ty = lax.axis_index("dp"), lax.axis_index("tx"), lax.axis_index("ty")
    c, x = ty % 2, ty // 2
    images, width, tokens = xg.shape
    cols = h.shape[1]
    half, quarter, eighth = width // 2, width // 4, width // 8
    rows_q = 3 * wq_hbm.shape[1] // 3
    head = v3.shape[1]
    heads = v3.shape[0]
    units = wup.shape[2]
    sib = (dp, y, ty + 1 - 2 * c)
    across = (dp, y, (ty + 2) % 4)
    row = (dp, 1 - y, ty)

    barrier = pltpu.get_barrier_semaphore()
    for peer in (sib, across, row, (dp, y, 3 - ty), (dp, 1 - y, ty + 1 - 2 * c)):
        pl.semaphore_signal(barrier, inc=1, device_id=peer, device_id_type=MESH)

    def send(src, dst, ssem, rsem, peer):
        return pltpu.make_async_remote_copy(src_ref=src, dst_ref=dst, send_sem=ssem, recv_sem=rsem,
                                            device_id=peer, device_id_type=MESH)

    def pieces(l):
        res = []
        for t, w in enumerate((wq_hbm, wk_hbm, wv_hbm)):
            res.append((w.at[l], wqkv.at[l, y, pl.ds(rows_q * t, rows_q)]))
        res.append((wup_hbm.at[l], wup.at[l, pl.ds(half * y, half)]))
        res.append((wdn_hbm.at[l], wdn.at[l, pl.ds(half * y, half)]))
        return res

    def w_local(l, n):
        src, dst = pieces(l)[n]
        return pltpu.make_async_copy(src, dst, loc_sem.at[l, n])

    def w_remote(l, n):
        src, dst = pieces(l)[n]
        return send(src, dst, ws_sem.at[l, n], wr_sem.at[l, n], row)

    def w_wait(l, ns):
        for n in ns:
            w_local(l, n).wait()
            w_remote(l, n).wait_recv()

    def wo_send(l, kind):
        peer = ((dp, y, 2 * x + y), (dp, y, 2 * (1 - x) + y), (dp, 1 - y, 2 * x + y))[kind]
        return send(wo_hbm.at[l], wo.at[l, ty], wo_s.at[l, kind], wo_r.at[l, ty], peer)

    def wo_local(l):
        return pltpu.make_async_copy(wo_hbm.at[l], wo.at[l, ty], wo_loc.at[l])

    def wo_here(l):
        @pl.when(c == y)
        def _():
            wo_local(l).start()

        @pl.when(c != y)
        def _():
            wo_send(l, 0).start()

    def wo_pass(l, n):
        ref = wo.at[l, 2 * x + n]
        return send(ref, ref, wo_s.at[l, 3 + n], wo_r.at[l, 2 * x + n], across)

    def wo_came(l, block):
        send(wo_hbm.at[l], wo.at[l, block], wo_s.at[l, 0], wo_r.at[l, block], across).wait_recv()

    def wo_fwd(l):
        @pl.when(c != y)
        def _():
            for n in range(2):
                wo_came(l, 2 * x + n)
                wo_pass(l, n).start()

    def wo_wait(l):
        for n in range(2):
            wo_came(l, 2 * (1 - x) + n)

        @pl.when(c == y)
        def _():
            wo_local(l).wait()
            wo_came(l, ty + 1 - 2 * c)

    def wo_end(l):
        for kind in (1, 2):
            wo_send(l, kind).wait_send()

        @pl.when(c != y)
        def _():
            wo_send(l, 0).wait_send()
            for n in range(2):
                wo_pass(l, n).wait_send()

    def mine_in(i):
        return pltpu.make_async_copy(x_hbm.at[y * images + i], xg.at[i, pl.ds(half * y, half)], x_sem.at[i])

    def entry_row(i):
        at = eighth * (2 * c + x)
        return send(x_hbm.at[(1 - y) * images + i, pl.ds(at, eighth)],
                    xg.at[i, pl.ds(half * y + at, eighth)], en_s.at[0, i], en_r.at[0, i], row)

    def entry_fwd(kind, i):
        src_x = x if kind < 3 else 1 - x
        ref = xg.at[i, pl.ds(half * (1 - y) + eighth * (2 * c + src_x), eighth)]
        return send(ref, ref, en_s.at[kind, i], en_r.at[kind, i], across if kind == 1 else sib)

    def entry(i):
        entry_row(i).wait_recv()
        entry_fwd(1, i).start()
        entry_fwd(2, i).start()
        entry_fwd(1, i).wait_recv()
        entry_fwd(3, i).start()

    def entry_done(i):
        mine_in(i).wait()
        entry_fwd(2, i).wait_recv()
        entry_fwd(3, i).wait_recv()
        entry_row(i).wait_send()
        for kind in (1, 2, 3):
            entry_fwd(kind, i).wait_send()

    def d2d(i):
        return send(part.at[pl.ds(half * (1 - c), half)], rd.at[i], d2_s.at[i], d2_r.at[i], sib)

    cut = quarter // CUTS

    def scatter(i, j):
        at = pl.ds(cut * j, cut)
        return send(rs.at[i, at], rr.at[i, at], rs_s.at[i, j], rs_r.at[i, j], across)

    def gather(kind, i):
        src_x = x if kind < 2 else 1 - x
        ref = xg.at[i, pl.ds(half * c + quarter * src_x, quarter)]
        return send(ref, ref, ag_s.at[kind, i], ag_r.at[kind, i], across if kind == 0 else sib)

    def stage_b(k, slot):
        i = k % images
        d2d(i).wait_recv()
        mine, theirs = quarter * x, quarter * (1 - x)
        acc[i] = (part[pl.ds(pl.multiple_of(half * slot + mine, 16), quarter)].astype(F32)
                  + rd[i, pl.ds(pl.multiple_of(mine, 16), quarter)].astype(F32))
        rs[i] = (part[pl.ds(pl.multiple_of(half * slot + theirs, 16), quarter)].astype(F32)
                 + rd[i, pl.ds(pl.multiple_of(theirs, 16), quarter)].astype(F32)).astype(BF16)
        for j in range(CUTS):
            scatter(i, j).start()

    def column(ref, at, size, lane):
        block = ref[pl.ds(at, size), :]
        picked = jnp.where(lax.broadcasted_iota(jnp.int32, block.shape, 1) == lane, block, 0.0)
        return jnp.sum(picked, axis=1, keepdims=True)

    def out_piece(own_row, i, j, at_x):
        image = (y if own_row else 1 - y) * images + i
        return out_hbm.at[image, pl.ds(quarter * at_x + cut * j, cut)]

    def final_piece(i, j):
        return xg.at[i, pl.ds(half * c + quarter * x + cut * j, cut)]

    def exit_copy(kind, i, j):
        sems = (ex_s.at[kind, i, j], ex_r.at[kind, i, j])
        if kind == 0:
            return send(final_piece(i, j), out_piece(True, i, j, x), *sems, row)
        if kind in (1, 2):
            return send(final_piece(i, j), out_piece(True, i, j, x), *sems, across if kind == 1 else sib)
        if kind in (3, 4):
            ref = out_piece(False, i, j, x)
            return send(ref, ref, *sems, across if kind == 3 else sib)
        ref = out_piece(kind == 5, i, j, 1 - x)
        return send(ref, ref, *sems, sib)

    def exit_local(i, j):
        return pltpu.make_async_copy(final_piece(i, j), out_piece(True, i, j, x), lo_sem.at[i, j])

    def stage_c(k):
        i, s = k % images, k // images
        for j in range(CUTS):
            scatter(i, j).wait_recv()
            at = pl.multiple_of(half * c + quarter * x + cut * j, 16)
            bias = column(vt, at, cut, 8 + s)
            got = acc[i, cut * j:cut * (j + 1)] + rr[i, cut * j:cut * (j + 1)].astype(F32)
            new = xg[i, pl.ds(at, cut)].astype(F32) + got[:, :tokens] + bias
            xg[i, pl.ds(at, cut)] = new.astype(BF16)

            @pl.when((s == 3) & (c == y))
            def _():
                exit_copy(1, i, j).start()
                exit_copy(2, i, j).start()
                exit_local(i, j).start()

            @pl.when((s == 3) & (c != y))
            def _():
                exit_copy(0, i, j).start()

        for j in range(CUTS):
            scatter(i, j).wait_send()

        @pl.when(s < 3)
        def _():
            gather(0, i).start()
            gather(1, i).start()

    def exit_row(i):
        @pl.when(c == y)
        def _():
            for j in range(CUTS):
                send(final_piece(i, j), out_piece(False, i, j, x), ex_s.at[0, i, j], ex_r.at[0, i, j], row).wait_recv()
                exit_copy(3, i, j).start()
                exit_copy(4, i, j).start()

    def exit_across(i, own_row):
        kind = 1 if own_row else 3

        @pl.when(c == y)
        def _():
            for j in range(CUTS):
                piece = out_piece(own_row, i, j, 1 - x)
                send(piece, piece, ex_s.at[kind, i, j], ex_r.at[kind, i, j], across).wait_recv()
                exit_copy(5 if own_row else 6, i, j).start()

    def stage_d(k):
        i = k % images
        gather(0, i).wait_recv()
        gather(2, i).start()

    def gather_done(k):
        i = k % images
        gather(1, i).wait_recv()
        gather(2, i).wait_recv()
        for kind in (0, 1, 2):
            gather(kind, i).wait_send()

    def norm(i, s):
        blocks = [pl.ds(b * quarter, quarter) for b in range(4)]
        total = sum(jnp.sum(xg[i, b].astype(F32), axis=0, keepdims=True) for b in blocks)
        mean = total / width
        spread = jnp.zeros_like(mean)
        for b in blocks:
            d = xg[i, b].astype(F32) - mean
            spread = spread + jnp.sum(d * d, axis=0, keepdims=True)
        inv = lax.rsqrt(spread / width + EPS)
        for n, b in enumerate(blocks):
            gain, shift = column(vt, n * quarter, quarter, s), column(vt, n * quarter, quarter, 4 + s)
            h[b, 0:tokens] = ((xg[i, b].astype(F32) - mean) * inv * gain + shift).astype(BF16)

    factor = (head ** -0.5) * 1.4426950408889634

    def attend(l, i):
        @pl.when(i == 0)
        def _():
            w_wait(l, (0, 1, 2))
        norm(i, 2 * l)
        for t, ref in enumerate((q3, k3, v3)):
            at = pl.ds(rows_q * t, rows_q)
            value = nn_dot(wqkv[l, 0, at], h[:half]) + nn_dot(wqkv[l, 1, at], h[half:])
            for n in range(heads):
                one = value[n * head:(n + 1) * head]
                if t != 1:
                    one = one + column(ct, 0, head, heads * (t + l) + n)
                ref[n, 0:head, :] = one.astype(BF16)

        edge, top = -(-tokens // 16) * 16, tokens // 16 * 16

        def one_head(n, _):
            s = nn_dot(k3[n].T[:edge], q3[n])
            tail = s[top:]
            tail = jnp.where(lax.broadcasted_iota(jnp.int32, tail.shape, 0) + top < tokens, tail, -1e30)
            s = jnp.concatenate([s[:top], tail], axis=0)
            e = jnp.exp2((s - jnp.max(s, axis=0, keepdims=True)) * factor)
            p = (e * (1.0 / jnp.sum(e, axis=0, keepdims=True))).astype(BF16)
            att[n] = nn_dot(v3[n, :, :edge], p)
            return 0
        lax.fori_loop(0, heads, one_head, 0, unroll=4)

        packed = jnp.concatenate([att[n] for n in range(heads)], axis=0).astype(BF16)
        every[i, pl.ds(pl.multiple_of(rows_q * ty, 16), rows_q), :] = packed
        att_copy(0, i).start()
        att_copy(1, i).start()

    def att_copy(kind, i):
        owner = ty if kind < 2 else (ty + 2) % 4
        ref = every.at[i, pl.ds(rows_q * owner, rows_q)]
        return send(ref, ref, at_s.at[kind, i], at_r.at[kind, i], across if kind == 0 else sib)

    def half_copy(i):
        ref = xg.at[i, pl.ds(half * c, half)]
        return send(ref, ref, hx_s.at[i], hx_r.at[i], sib)

    def att_fwd(i):
        att_copy(0, i).wait_recv()
        att_copy(2, i).start()

    def att_out(l, i):
        if isinstance(i, int) and i == 0:
            wo_wait(l)
        att_copy(1, i).wait_recv()
        att_copy(2, i).wait_recv()
        at = pl.multiple_of(half * c, 16)
        value = tn_dot(wo[l].reshape(width, half), every[i]) + column(vt, at, half, 8 + 2 * l)
        xg[i, pl.ds(at, half)] = (xg[i, pl.ds(at, half)].astype(F32) + value[:, :tokens]).astype(BF16)
        half_copy(i).start()
        for kind in range(3):
            att_copy(kind, i).wait_send()

    def down(l, i, hf, slot):
        at = pl.multiple_of(half * hf, 16)
        part[pl.ds(pl.multiple_of(half * slot, 16), half)] = nn_dot(wdn[l, pl.ds(at, half)], every[i, 0:units]).astype(BF16)

    def mlp_first(l, i):
        k = 2 * images * l + images + i
        half_copy(i).wait_recv()
        half_copy(i).wait_send()
        @pl.when(i == 0)
        def _():
            w_wait(l, (3,))
        norm(i, 2 * l + 1)
        for a in range(0, units, 640):
            b = min(units, a + 640)
            u = tn_dot(wup[l, :, a:b], h[...]) + column(ut, a, b - a, l)
            every[i, a:b, :] = gelu(u).astype(BF16)

        @pl.when(i == 0)
        def _():
            att_fwd(images - 1)
            att_out(l, images - 1)
            w_local(l, 4).wait()

        @pl.when((c == y) & (i >= 1))
        def _():
            stage_b(k - 1, c)

        @pl.when((c == y) & (i >= 2))
        def _():
            stage_c(k - 2)

        @pl.when((c != y) & (i >= 1))
        def _():
            d2d(i - 1).wait_send()
        down(l, i, y, y)

        @pl.when(c != y)
        def _():
            d2d(i).start()

    def mlp_second(l, i):
        k = 2 * images * l + images + i

        @pl.when(i == 0)
        def _():
            @pl.when(c == y)
            def _():
                stage_b(k + images - 1, c)
                stage_c(k + images - 2)

            @pl.when(c != y)
            def _():
                d2d(images - 1).wait_send()
            w_remote(l, 4).wait_recv()

        @pl.when((c == y) & (i >= 1))
        def _():
            d2d(i - 1).wait_send()
        down(l, i, 1 - y, (1 - y + i * (c + y - 2 * c * y)) % 2)

        @pl.when(c == y)
        def _():
            d2d(i).start()

            @pl.when(i == 1)
            def _():
                stage_c(k + images - 2)

            @pl.when(i >= 1)
            def _():
                send_on(l, k - 1)

        @pl.when((c != y) & (i >= 1))
        def _():
            stage_b(k - 1, (c + i - 1) % 2)

        @pl.when((c != y) & (i >= 2))
        def _():
            stage_c(k - 2)

    def send_on(l, k):
        @pl.when(l == 0)
        def _():
            stage_d(k)

        @pl.when(l == 1)
        def _():
            exit_across(k % images, True)

    def mlp_end(l):
        k = 2 * images * l + 2 * images - 1

        @pl.when(c == y)
        def _():
            d2d(images - 1).wait_send()
            send_on(l, k)

        @pl.when(c != y)
        def _():
            stage_b(k, (c + images - 1) % 2)
            stage_c(k - 1)

            @pl.when(l == 0)
            def _():
                stage_d(k - 2)

    for i in range(images):
        mine_in(i).start()
    for n in range(5):
        w_local(0, n).start()
    vecs = (g1_hbm, g2_hbm, s1_hbm, s2_hbm, bo_hbm, bd_hbm)
    small = [pltpu.make_async_copy(v, vraw.at[y, n], vec_sem.at[n]) for n, v in enumerate(vecs)]
    small += [pltpu.make_async_copy(b, craw.at[n], vec_sem.at[6 + n]) for n, b in enumerate((bq_hbm, bv_hbm))]
    small.append(pltpu.make_async_copy(bup_hbm, uraw, vec_sem.at[8]))
    for copy in small:
        copy.start()
    vec_row = [send(v, vraw.at[y, n], vec_s.at[n], vec_r.at[n], row) for n, v in enumerate(vecs)]
    pl.semaphore_wait(barrier, 5)
    entry_row(0).start()
    for copy in vec_row:
        copy.start()
    wo_here(0)
    wo_send(0, 1).start()
    for n in range(3):
        w_remote(0, n).start()
    wo_send(0, 2).start()
    for i in range(1, images):
        entry_row(i).start()
    for n in range(3, 5):
        w_remote(0, n).start()
    wo_here(1)
    wo_send(1, 1).start()
    for n in range(5):
        w_local(1, n).start()

    layers = wup.shape[0]
    for ref in (vpad, cpad, upad):
        ref[...] = jnp.zeros_like(ref)
    h[:, cols - 128:] = jnp.zeros((width, 128), BF16)
    q3[:, head:, :] = jnp.zeros((heads, q3.shape[1] - head, cols), BF16)
    k3[:, head:, :] = jnp.zeros((heads, k3.shape[1] - head, cols), BF16)
    for copy in small:
        copy.wait()
    for l in range(layers):
        upad[l:l + 1, 0:uraw.shape[1]] = uraw[l:l + 1, :]
        for t in range(2):
            at = (2 * t + l) * heads
            cpad[at:at + heads, 0:head] = craw[t, l]
    ct[...] = cpad[...].T
    ut[...] = upad[...].T
    for copy in vec_row:
        copy.wait()
    for n in range(2):
        for a in range(6):
            for l in range(layers):
                at = 4 * (a // 2) + 2 * l + a % 2
                vpad[n, at:at + 1, 0:half] = vraw[n, a, l:l + 1, :]
        vt[n * half:(n + 1) * half, :] = vpad[n].T[:half]
    entry(0)

    def layer(l, _):
        def attn_step(i, _):
            k = 2 * images * l + i

            @pl.when(l == 0)
            def _():
                entry_done(i)

            @pl.when(l > 0)
            def _():
                gather_done(k)
            attend(l, i)

            @pl.when(i >= 1)
            def _():
                att_fwd(i - 1)

            @pl.when((l > 0) & (i == 0) & (c != y))
            def _():
                stage_c(k - 1)

            @pl.when((l > 0) & (i <= 1) & (c != y))
            def _():
                stage_d(k - 2)

            @pl.when(i == 0)
            def _():
                wo_fwd(l)

            @pl.when(k == 0)
            def _():
                for j in range(1, images):
                    entry(j)
                for n in range(3):
                    w_remote(1, n).start()
                wo_send(1, 2).start()
                for n in range(3, 5):
                    w_remote(1, n).start()

            @pl.when(i == images - 1)
            def _():
                for j in range(images - 1):
                    att_out(l, j)
            return 0
        lax.fori_loop(0, images, attn_step, 0)

        def first_step(i, _):
            mlp_first(l, i)
            return 0
        lax.fori_loop(0, images, first_step, 0)

        def second_step(i, _):
            mlp_second(l, i)
            return 0
        lax.fori_loop(0, images, second_step, 0)

        mlp_end(l)
        return 0
    lax.fori_loop(0, 2, layer, 0)

    @pl.when(c != y)
    def _():
        stage_c(4 * images - 1)
    for i in range(images):
        exit_row(i)
        if i >= 1:
            exit_across(i - 1, False)
    exit_across(images - 1, False)

    @pl.when(c == y)
    def _():
        for i in range(images):
            for j in range(CUTS):
                exit_local(i, j).wait()
                for kind in (1, 2, 3, 4, 5, 6):
                    exit_copy(kind, i, j).wait_send()

    @pl.when(c != y)
    def _():
        for i in range(images):
            for j in range(CUTS):
                exit_copy(0, i, j).wait_send()
                for kind, own_row, at_x in ((2, True, x), (4, False, x), (5, True, 1 - x), (6, False, 1 - x)):
                    piece = out_piece(own_row, i, j, at_x)
                    send(piece, piece, ex_s.at[kind, i, j], ex_r.at[kind, i, j], sib).wait_recv()
    for l in range(2):
        wo_end(l)
        for n in range(5):
            w_remote(l, n).wait_send()


def solution(mesh):
    act_spec = P("dp", None, "tx")
    vec_tx = P(None, "tx")
    proj_spec = P(None, "tx", "ty", None)
    head_vec = P(None, "ty", None)
    in_specs = (act_spec, vec_tx, vec_tx, proj_spec, head_vec, proj_spec, proj_spec, head_vec,
                P(None, "ty", None, "tx"), vec_tx, vec_tx, vec_tx,
                P(None, "tx", "ty"), P(None, "ty"), P(None, "ty", "tx"), vec_tx)

    def local_fn(x_in, ln1_gain, ln1_bias, w_q, b_q, w_k, w_v, b_v, w_o, b_o, ln2_gain, ln2_bias, w_up, b_up, w_down, b_down):
        total, tokens, half = x_in.shape
        layers, _, heads, head = w_q.shape
        units = w_up.shape[2]
        images, width, rows_q = total // 2, 2 * half, heads * head
        cols = -(-tokens // 256) * 256
        lanes = -(-half // 128) * 128
        long = -(-units // 128) * 128
        flat = lambda w: w.reshape(layers, half, rows_q).transpose(0, 2, 1)
        dma = pltpu.SemaphoreType.DMA
        vmem = pltpu.VMEM
        y_t = pl.pallas_call(
            kernel,
            out_shape=jax.ShapeDtypeStruct((total, half, tokens), BF16),
            in_specs=[pl.BlockSpec(memory_space=pl.ANY)] * 16,
            out_specs=pl.BlockSpec(memory_space=pl.ANY),
            scratch_shapes=[
                vmem((images, width, tokens), BF16), vmem((width, cols), BF16), vmem((width, cols), BF16),
                vmem((images, half, cols), BF16), vmem((images, half // 2, cols), BF16),
                vmem((images, half // 2, cols), BF16), vmem((images, half // 2, cols), F32),
                vmem((heads, 128, cols), BF16), vmem((heads, 128, cols), BF16), vmem((heads, head, cols), BF16),
                vmem((heads, head, cols), F32), vmem((images, width, cols), BF16),
                vmem((layers, 2, 3 * rows_q, half), BF16), vmem((layers, 4, rows_q, half), BF16),
                vmem((layers, width, units), BF16), vmem((layers, width, units), BF16),
                vmem((2, 6, layers, half), F32), vmem((2, layers, heads, head), F32), vmem((layers, units), F32),
                vmem((2, 128, lanes), F32), vmem((128, 128), F32), vmem((128, long), F32),
                vmem((width, 128), F32), vmem((128, 128), F32), vmem((long, 128), F32),
                dma((2, 5)), dma((2, 5)), dma((2, 5)), dma((9,)), dma((6,)), dma((6,)), dma((images,)),
                dma((4, images)), dma((4, images)), dma((images,)), dma((images,)),
                dma((images, CUTS)), dma((images, CUTS)), dma((3, images)), dma((3, images)),
                dma((7, images, CUTS)), dma((7, images, CUTS)), dma((images, CUTS)),
                dma((3, images)), dma((3, images)), dma((images,)), dma((images,)), dma((2,)), dma((2, 5)), dma((2, 4)),
            ],
            compiler_params=pltpu.CompilerParams(collective_id=0, has_side_effects=True, vmem_limit_bytes=66_000_000),
            name="encoder",
        )(x_in.transpose(0, 2, 1), ln1_gain, ln2_gain, ln1_bias, ln2_bias, b_o, b_down, b_q, b_v, b_up,
          flat(w_q), flat(w_k), flat(w_v), w_o.reshape(layers, rows_q, half), w_up, w_down.transpose(0, 2, 1))
        return y_t.transpose(0, 2, 1)

    return jax.shard_map(local_fn, mesh=mesh, in_specs=in_specs, out_specs=act_spec, check_vma=False)
```

```python
import jax
import jax.numpy as jnp
from jax import lax
from jax.experimental import pallas as pl
from jax.experimental.pallas import tpu as pltpu
from jax.sharding import PartitionSpec as P

EPS = 1e-6
MESH = pl.DeviceIdType.MESH
F32, BF16 = jnp.float32, jnp.bfloat16
CUTS = 3


def tn_dot(a, b):
    return lax.dot_general(a, b, (((0,), (0,)), ((), ())), preferred_element_type=F32)


def nn_dot(a, b):
    return jnp.dot(a, b, preferred_element_type=F32)


def gelu(u):
    return 0.5 * u * (1.0 + jnp.tanh(0.7978845608028654 * (u + 0.044715 * u * u * u)))


def kernel(x_hbm, g1_hbm, g2_hbm, s1_hbm, s2_hbm, bo_hbm, bd_hbm, bq_hbm, bv_hbm, bup_hbm, wq_hbm, wk_hbm, wv_hbm, wo_hbm, wup_hbm, wdn_hbm, out_hbm,
           xg, h, part, rd, rs, rr, acc, q3, k3, v3, att, every, wqkv, wo, wup, wdn, vraw, craw, uraw, vpad, cpad, upad, vt, ct, ut,
           loc_sem, ws_sem, wr_sem, vec_sem, vec_s, vec_r, x_sem, en_s, en_r, d2_s, d2_r, rs_s, rs_r, ag_s, ag_r, ex_s, ex_r, lo_sem,
           at_s, at_r, hx_s, hx_r, wo_loc, wo_s, wo_r):
    dp, y, ty = lax.axis_index("dp"), lax.axis_index("tx"), lax.axis_index("ty")
    c, x = ty % 2, ty // 2
    images, width, tokens = xg.shape
    cols = h.shape[1]
    half, quarter, eighth = width // 2, width // 4, width // 8
    rows_q = 3 * wq_hbm.shape[1] // 3
    head = v3.shape[1]
    heads = v3.shape[0]
    units = wup.shape[2]
    sib = (dp, y, ty + 1 - 2 * c)
    across = (dp, y, (ty + 2) % 4)
    row = (dp, 1 - y, ty)

    barrier = pltpu.get_barrier_semaphore()
    for peer in (sib, across, row, (dp, y, 3 - ty), (dp, 1 - y, ty + 1 - 2 * c)):
        pl.semaphore_signal(barrier, inc=1, device_id=peer, device_id_type=MESH)

    def send(src, dst, ssem, rsem, peer):
        return pltpu.make_async_remote_copy(src_ref=src, dst_ref=dst, send_sem=ssem, recv_sem=rsem,
                                            device_id=peer, device_id_type=MESH)

    def pieces(l):
        res = []
        for t, w in enumerate((wq_hbm, wk_hbm, wv_hbm)):
            res.append((w.at[l], wqkv.at[l, y, pl.ds(rows_q * t, rows_q)]))
        res.append((wup_hbm.at[l], wup.at[l, pl.ds(half * y, half)]))
        res.append((wdn_hbm.at[l], wdn.at[l, pl.ds(half * y, half)]))
        return res

    def w_local(l, n):
        src, dst = pieces(l)[n]
        return pltpu.make_async_copy(src, dst, loc_sem.at[l, n])

    def w_remote(l, n):
        src, dst = pieces(l)[n]
        return send(src, dst, ws_sem.at[l, n], wr_sem.at[l, n], row)

    def w_wait(l, ns):
        for n in ns:
            w_local(l, n).wait()
            w_remote(l, n).wait_recv()

    def wo_send(l, kind):
        peer = ((dp, y, 2 * x + y), (dp, y, 2 * (1 - x) + y), (dp, 1 - y, 2 * x + y))[kind]
        return send(wo_hbm.at[l], wo.at[l, ty], wo_s.at[l, kind], wo_r.at[l, ty], peer)

    def wo_local(l):
        return pltpu.make_async_copy(wo_hbm.at[l], wo.at[l, ty], wo_loc.at[l])

    def wo_here(l):
        @pl.when(c == y)
        def _():
            wo_local(l).start()

        @pl.when(c != y)
        def _():
            wo_send(l, 0).start()

    def wo_pass(l, n):
        ref = wo.at[l, 2 * x + n]
        return send(ref, ref, wo_s.at[l, 3 + n], wo_r.at[l, 2 * x + n], across)

    def wo_came(l, block):
        send(wo_hbm.at[l], wo.at[l, block], wo_s.at[l, 0], wo_r.at[l, block], across).wait_recv()

    def wo_fwd(l):
        @pl.when(c != y)
        def _():
            for n in range(2):
                wo_came(l, 2 * x + n)
                wo_pass(l, n).start()

    def wo_wait(l):
        for n in range(2):
            wo_came(l, 2 * (1 - x) + n)

        @pl.when(c == y)
        def _():
            wo_local(l).wait()
            wo_came(l, ty + 1 - 2 * c)

    def wo_end(l):
        for kind in (1, 2):
            wo_send(l, kind).wait_send()

        @pl.when(c != y)
        def _():
            wo_send(l, 0).wait_send()
            for n in range(2):
                wo_pass(l, n).wait_send()

    def mine_in(i):
        return pltpu.make_async_copy(x_hbm.at[y * images + i], xg.at[i, pl.ds(half * y, half)], x_sem.at[i])

    def entry_row(i):
        at = eighth * (2 * c + x)
        return send(x_hbm.at[(1 - y) * images + i, pl.ds(at, eighth)],
                    xg.at[i, pl.ds(half * y + at, eighth)], en_s.at[0, i], en_r.at[0, i], row)

    def entry_fwd(kind, i):
        src_x = x if kind < 3 else 1 - x
        ref = xg.at[i, pl.ds(half * (1 - y) + eighth * (2 * c + src_x), eighth)]
        return send(ref, ref, en_s.at[kind, i], en_r.at[kind, i], across if kind == 1 else sib)

    def entry(i):
        entry_row(i).wait_recv()
        entry_fwd(1, i).start()
        entry_fwd(2, i).start()
        entry_fwd(1, i).wait_recv()
        entry_fwd(3, i).start()

    def entry_done(i):
        mine_in(i).wait()
        entry_fwd(2, i).wait_recv()
        entry_fwd(3, i).wait_recv()
        entry_row(i).wait_send()
        for kind in (1, 2, 3):
            entry_fwd(kind, i).wait_send()

    def d2d(i):
        return send(part.at[pl.ds(half * (1 - c), half)], rd.at[i], d2_s.at[i], d2_r.at[i], sib)

    cut = quarter // CUTS

    def scatter(i, j):
        at = pl.ds(cut * j, cut)
        return send(rs.at[i, at], rr.at[i, at], rs_s.at[i, j], rs_r.at[i, j], across)

    def gather(kind, i):
        src_x = x if kind < 2 else 1 - x
        ref = xg.at[i, pl.ds(half * c + quarter * src_x, quarter)]
        return send(ref, ref, ag_s.at[kind, i], ag_r.at[kind, i], across if kind == 0 else sib)

    def stage_b(k, slot):
        i = k % images
        d2d(i).wait_recv()
        mine, theirs = quarter * x, quarter * (1 - x)
        for j in range(CUTS):
            rows = pl.ds(cut * j, cut)
            rs[i, rows] = (part[pl.ds(pl.multiple_of(half * slot + theirs + cut * j, 16), cut)].astype(F32)
                           + rd[i, pl.ds(pl.multiple_of(theirs + cut * j, 16), cut)].astype(F32)).astype(BF16)
            scatter(i, j).start()
        acc[i] = (part[pl.ds(pl.multiple_of(half * slot + mine, 16), quarter)].astype(F32)
                  + rd[i, pl.ds(pl.multiple_of(mine, 16), quarter)].astype(F32))

    def column(ref, at, size, lane):
        block = ref[pl.ds(at, size), :]
        picked = jnp.where(lax.broadcasted_iota(jnp.int32, block.shape, 1) == lane, block, 0.0)
        return jnp.sum(picked, axis=1, keepdims=True)

    def out_piece(own_row, i, j, at_x):
        image = (y if own_row else 1 - y) * images + i
        return out_hbm.at[image, pl.ds(quarter * at_x + cut * j, cut)]

    def final_piece(i, j):
        return xg.at[i, pl.ds(half * c + quarter * x + cut * j, cut)]

    def exit_copy(kind, i, j):
        sems = (ex_s.at[kind, i, j], ex_r.at[kind, i, j])
        if kind == 0:
            return send(final_piece(i, j), out_piece(True, i, j, x), *sems, row)
        if kind in (1, 2):
            return send(final_piece(i, j), out_piece(True, i, j, x), *sems, across if kind == 1 else sib)
        if kind in (3, 4):
            ref = out_piece(False, i, j, x)
            return send(ref, ref, *sems, across if kind == 3 else sib)
        ref = out_piece(kind == 5, i, j, 1 - x)
        return send(ref, ref, *sems, sib)

    def exit_local(i, j):
        return pltpu.make_async_copy(final_piece(i, j), out_piece(True, i, j, x), lo_sem.at[i, j])

    def stage_c(k):
        i, s = k % images, k // images
        for j in range(CUTS):
            scatter(i, j).wait_recv()
            at = pl.multiple_of(half * c + quarter * x + cut * j, 16)
            bias = column(vt, at, cut, 8 + s)
            got = acc[i, cut * j:cut * (j + 1)] + rr[i, cut * j:cut * (j + 1)].astype(F32)
            new = xg[i, pl.ds(at, cut)].astype(F32) + got[:, :tokens] + bias
            xg[i, pl.ds(at, cut)] = new.astype(BF16)

            @pl.when((s == 3) & (c == y))
            def _():
                exit_copy(1, i, j).start()
                exit_copy(2, i, j).start()
                exit_local(i, j).start()

            @pl.when((s == 3) & (c != y))
            def _():
                exit_copy(0, i, j).start()

        for j in range(CUTS):
            scatter(i, j).wait_send()

        @pl.when(s < 3)
        def _():
            gather(0, i).start()
            gather(1, i).start()

    def exit_row(i):
        @pl.when(c == y)
        def _():
            for j in range(CUTS):
                send(final_piece(i, j), out_piece(False, i, j, x), ex_s.at[0, i, j], ex_r.at[0, i, j], row).wait_recv()
                exit_copy(3, i, j).start()
                exit_copy(4, i, j).start()

    def exit_across(i, own_row):
        kind = 1 if own_row else 3

        @pl.when(c == y)
        def _():
            for j in range(CUTS):
                piece = out_piece(own_row, i, j, 1 - x)
                send(piece, piece, ex_s.at[kind, i, j], ex_r.at[kind, i, j], across).wait_recv()
                exit_copy(5 if own_row else 6, i, j).start()

    def stage_d(k):
        i = k % images
        gather(0, i).wait_recv()
        gather(2, i).start()

    def gather_done(k):
        i = k % images
        gather(1, i).wait_recv()
        gather(2, i).wait_recv()
        for kind in (0, 1, 2):
            gather(kind, i).wait_send()

    def norm(i, s):
        blocks = [pl.ds(b * quarter, quarter) for b in range(4)]
        total = sum(jnp.sum(xg[i, b].astype(F32), axis=0, keepdims=True) for b in blocks)
        mean = total / width
        spread = jnp.zeros_like(mean)
        for b in blocks:
            d = xg[i, b].astype(F32) - mean
            spread = spread + jnp.sum(d * d, axis=0, keepdims=True)
        inv = lax.rsqrt(spread / width + EPS)
        for n, b in enumerate(blocks):
            gain, shift = column(vt, n * quarter, quarter, s), column(vt, n * quarter, quarter, 4 + s)
            h[b, 0:tokens] = ((xg[i, b].astype(F32) - mean) * inv * gain + shift).astype(BF16)

    factor = (head ** -0.5) * 1.4426950408889634

    def attend(l, i):
        @pl.when(i == 0)
        def _():
            w_wait(l, (0, 1, 2))
        norm(i, 2 * l)
        for t, ref in enumerate((q3, k3, v3)):
            at = pl.ds(rows_q * t, rows_q)
            value = nn_dot(wqkv[l, 0, at], h[:half]) + nn_dot(wqkv[l, 1, at], h[half:])
            for n in range(heads):
                one = value[n * head:(n + 1) * head]
                if t != 1:
                    one = one + column(ct, 0, head, heads * (t + l) + n)
                ref[n, 0:head, :] = one.astype(BF16)

        edge, top = -(-tokens // 16) * 16, tokens // 16 * 16

        def one_head(n, _):
            s = nn_dot(k3[n].T[:edge], q3[n])
            tail = s[top:]
            tail = jnp.where(lax.broadcasted_iota(jnp.int32, tail.shape, 0) + top < tokens, tail, -1e30)
            s = jnp.concatenate([s[:top], tail], axis=0)
            e = jnp.exp2((s - jnp.max(s, axis=0, keepdims=True)) * factor)
            p = (e * (1.0 / jnp.sum(e, axis=0, keepdims=True))).astype(BF16)
            att[n] = nn_dot(v3[n, :, :edge], p)
            return 0
        lax.fori_loop(0, heads, one_head, 0, unroll=4)

        packed = jnp.concatenate([att[n] for n in range(heads)], axis=0).astype(BF16)
        every[i, pl.ds(pl.multiple_of(rows_q * ty, 16), rows_q), :] = packed
        att_copy(0, i).start()
        att_copy(1, i).start()

    def att_copy(kind, i):
        owner = ty if kind < 2 else (ty + 2) % 4
        ref = every.at[i, pl.ds(rows_q * owner, rows_q)]
        return send(ref, ref, at_s.at[kind, i], at_r.at[kind, i], across if kind == 0 else sib)

    def half_copy(i):
        ref = xg.at[i, pl.ds(half * c, half)]
        return send(ref, ref, hx_s.at[i], hx_r.at[i], sib)

    def att_fwd(i):
        att_copy(0, i).wait_recv()
        att_copy(2, i).start()

    def att_out(l, i):
        if isinstance(i, int) and i == 0:
            wo_wait(l)
        att_copy(1, i).wait_recv()
        att_copy(2, i).wait_recv()
        at = pl.multiple_of(half * c, 16)
        value = tn_dot(wo[l].reshape(width, half), every[i]) + column(vt, at, half, 8 + 2 * l)
        xg[i, pl.ds(at, half)] = (xg[i, pl.ds(at, half)].astype(F32) + value[:, :tokens]).astype(BF16)
        half_copy(i).start()
        for kind in range(3):
            att_copy(kind, i).wait_send()

    def down(l, i, hf, slot):
        at = pl.multiple_of(half * hf, 16)
        part[pl.ds(pl.multiple_of(half * slot, 16), half)] = nn_dot(wdn[l, pl.ds(at, half)], every[i, 0:units]).astype(BF16)

    def mlp_first(l, i):
        k = 2 * images * l + images + i
        half_copy(i).wait_recv()
        half_copy(i).wait_send()
        @pl.when(i == 0)
        def _():
            w_wait(l, (3,))
        norm(i, 2 * l + 1)
        for a in range(0, units, 640):
            b = min(units, a + 640)
            u = tn_dot(wup[l, :, a:b], h[...]) + column(ut, a, b - a, l)
            every[i, a:b, :] = gelu(u).astype(BF16)

        @pl.when(i == 0)
        def _():
            att_fwd(images - 1)
            att_out(l, images - 1)
            w_local(l, 4).wait()

        @pl.when((c == y) & (i >= 1))
        def _():
            stage_b(k - 1, c)

        @pl.when((c == y) & (i >= 2))
        def _():
            stage_c(k - 2)

        @pl.when((c != y) & (i >= 1))
        def _():
            d2d(i - 1).wait_send()
        down(l, i, y, y)

        @pl.when(c != y)
        def _():
            d2d(i).start()

    def mlp_second(l, i):
        k = 2 * images * l + images + i

        @pl.when(i == 0)
        def _():
            @pl.when(c == y)
            def _():
                stage_b(k + images - 1, c)
                stage_c(k + images - 2)

            @pl.when(c != y)
            def _():
                d2d(images - 1).wait_send()
            w_remote(l, 4).wait_recv()

        @pl.when((c == y) & (i >= 1))
        def _():
            d2d(i - 1).wait_send()
        down(l, i, 1 - y, (1 - y + i * (c + y - 2 * c * y)) % 2)

        @pl.when(c == y)
        def _():
            d2d(i).start()

            @pl.when(i == 1)
            def _():
                stage_c(k + images - 2)

            @pl.when(i >= 1)
            def _():
                send_on(l, k - 1)

        @pl.when((c != y) & (i >= 1))
        def _():
            stage_b(k - 1, (c + i - 1) % 2)

        @pl.when((c != y) & (i >= 2))
        def _():
            stage_c(k - 2)

    def send_on(l, k):
        @pl.when(l == 0)
        def _():
            stage_d(k)

        @pl.when(l == 1)
        def _():
            exit_across(k % images, True)

    def mlp_end(l):
        k = 2 * images * l + 2 * images - 1

        @pl.when(c == y)
        def _():
            d2d(images - 1).wait_send()
            send_on(l, k)

        @pl.when(c != y)
        def _():
            stage_b(k, (c + images - 1) % 2)
            stage_c(k - 1)

            @pl.when(l == 0)
            def _():
                stage_d(k - 2)

    for i in range(images):
        mine_in(i).start()
    for n in range(5):
        w_local(0, n).start()
    vecs = (g1_hbm, g2_hbm, s1_hbm, s2_hbm, bo_hbm, bd_hbm)
    small = [pltpu.make_async_copy(v, vraw.at[y, n], vec_sem.at[n]) for n, v in enumerate(vecs)]
    small += [pltpu.make_async_copy(b, craw.at[n], vec_sem.at[6 + n]) for n, b in enumerate((bq_hbm, bv_hbm))]
    small.append(pltpu.make_async_copy(bup_hbm, uraw, vec_sem.at[8]))
    for copy in small:
        copy.start()
    vec_row = [send(v, vraw.at[y, n], vec_s.at[n], vec_r.at[n], row) for n, v in enumerate(vecs)]
    pl.semaphore_wait(barrier, 5)
    entry_row(0).start()
    for copy in vec_row:
        copy.start()
    wo_here(0)
    wo_send(0, 1).start()
    for n in range(3):
        w_remote(0, n).start()
    wo_send(0, 2).start()
    for i in range(1, images):
        entry_row(i).start()
    for n in range(3, 5):
        w_remote(0, n).start()
    wo_here(1)
    wo_send(1, 1).start()
    for n in range(5):
        w_local(1, n).start()

    layers = wup.shape[0]
    for ref in (vpad, cpad, upad):
        ref[...] = jnp.zeros_like(ref)
    h[:, cols - 128:] = jnp.zeros((width, 128), BF16)
    q3[:, head:, :] = jnp.zeros((heads, q3.shape[1] - head, cols), BF16)
    k3[:, head:, :] = jnp.zeros((heads, k3.shape[1] - head, cols), BF16)
    for copy in small:
        copy.wait()
    for l in range(layers):
        upad[l:l + 1, 0:uraw.shape[1]] = uraw[l:l + 1, :]
        for t in range(2):
            at = (2 * t + l) * heads
            cpad[at:at + heads, 0:head] = craw[t, l]
    ct[...] = cpad[...].T
    ut[...] = upad[...].T
    for copy in vec_row:
        copy.wait()
    for n in range(2):
        for a in range(6):
            for l in range(layers):
                at = 4 * (a // 2) + 2 * l + a % 2
                vpad[n, at:at + 1, 0:half] = vraw[n, a, l:l + 1, :]
        vt[n * half:(n + 1) * half, :] = vpad[n].T[:half]
    entry(0)

    def layer(l, _):
        def attn_step(i, _):
            k = 2 * images * l + i

            @pl.when(l == 0)
            def _():
                entry_done(i)

            @pl.when(l > 0)
            def _():
                gather_done(k)
            attend(l, i)

            @pl.when(i >= 1)
            def _():
                att_fwd(i - 1)

            @pl.when((l > 0) & (i == 0) & (c != y))
            def _():
                stage_c(k - 1)

            @pl.when((l > 0) & (i <= 1) & (c != y))
            def _():
                stage_d(k - 2)

            @pl.when(i == 0)
            def _():
                wo_fwd(l)

            @pl.when(k == 0)
            def _():
                for j in range(1, images):
                    entry(j)
                for n in range(3):
                    w_remote(1, n).start()
                wo_send(1, 2).start()
                for n in range(3, 5):
                    w_remote(1, n).start()

            @pl.when(i == images - 1)
            def _():
                for j in range(images - 1):
                    att_out(l, j)
            return 0
        lax.fori_loop(0, images, attn_step, 0)

        def first_step(i, _):
            mlp_first(l, i)
            return 0
        lax.fori_loop(0, images, first_step, 0)

        def second_step(i, _):
            mlp_second(l, i)
            return 0
        lax.fori_loop(0, images, second_step, 0)

        mlp_end(l)
        return 0
    lax.fori_loop(0, 2, layer, 0)

    @pl.when(c != y)
    def _():
        stage_c(4 * images - 1)
    for i in range(images):
        exit_row(i)
        if i >= 1:
            exit_across(i - 1, False)
    exit_across(images - 1, False)

    @pl.when(c == y)
    def _():
        for i in range(images):
            for j in range(CUTS):
                exit_local(i, j).wait()
                for kind in (1, 2, 3, 4, 5, 6):
                    exit_copy(kind, i, j).wait_send()

    @pl.when(c != y)
    def _():
        for i in range(images):
            for j in range(CUTS):
                exit_copy(0, i, j).wait_send()
                for kind, own_row, at_x in ((2, True, x), (4, False, x), (5, True, 1 - x), (6, False, 1 - x)):
                    piece = out_piece(own_row, i, j, at_x)
                    send(piece, piece, ex_s.at[kind, i, j], ex_r.at[kind, i, j], sib).wait_recv()
    for l in range(2):
        wo_end(l)
        for n in range(5):
            w_remote(l, n).wait_send()


def solution(mesh):
    act_spec = P("dp", None, "tx")
    vec_tx = P(None, "tx")
    proj_spec = P(None, "tx", "ty", None)
    head_vec = P(None, "ty", None)
    in_specs = (act_spec, vec_tx, vec_tx, proj_spec, head_vec, proj_spec, proj_spec, head_vec,
                P(None, "ty", None, "tx"), vec_tx, vec_tx, vec_tx,
                P(None, "tx", "ty"), P(None, "ty"), P(None, "ty", "tx"), vec_tx)

    def local_fn(x_in, ln1_gain, ln1_bias, w_q, b_q, w_k, w_v, b_v, w_o, b_o, ln2_gain, ln2_bias, w_up, b_up, w_down, b_down):
        total, tokens, half = x_in.shape
        layers, _, heads, head = w_q.shape
        units = w_up.shape[2]
        images, width, rows_q = total // 2, 2 * half, heads * head
        cols = -(-tokens // 256) * 256
        lanes = -(-half // 128) * 128
        long = -(-units // 128) * 128
        flat = lambda w: w.reshape(layers, half, rows_q).transpose(0, 2, 1)
        dma = pltpu.SemaphoreType.DMA
        vmem = pltpu.VMEM
        y_t = pl.pallas_call(
            kernel,
            out_shape=jax.ShapeDtypeStruct((total, half, tokens), BF16),
            in_specs=[pl.BlockSpec(memory_space=pl.ANY)] * 16,
            out_specs=pl.BlockSpec(memory_space=pl.ANY),
            scratch_shapes=[
                vmem((images, width, tokens), BF16), vmem((width, cols), BF16), vmem((width, cols), BF16),
                vmem((images, half, cols), BF16), vmem((images, half // 2, cols), BF16),
                vmem((images, half // 2, cols), BF16), vmem((images, half // 2, cols), F32),
                vmem((heads, 128, cols), BF16), vmem((heads, 128, cols), BF16), vmem((heads, head, cols), BF16),
                vmem((heads, head, cols), F32), vmem((images, width, cols), BF16),
                vmem((layers, 2, 3 * rows_q, half), BF16), vmem((layers, 4, rows_q, half), BF16),
                vmem((layers, width, units), BF16), vmem((layers, width, units), BF16),
                vmem((2, 6, layers, half), F32), vmem((2, layers, heads, head), F32), vmem((layers, units), F32),
                vmem((2, 128, lanes), F32), vmem((128, 128), F32), vmem((128, long), F32),
                vmem((width, 128), F32), vmem((128, 128), F32), vmem((long, 128), F32),
                dma((2, 5)), dma((2, 5)), dma((2, 5)), dma((9,)), dma((6,)), dma((6,)), dma((images,)),
                dma((4, images)), dma((4, images)), dma((images,)), dma((images,)),
                dma((images, CUTS)), dma((images, CUTS)), dma((3, images)), dma((3, images)),
                dma((7, images, CUTS)), dma((7, images, CUTS)), dma((images, CUTS)),
                dma((3, images)), dma((3, images)), dma((images,)), dma((images,)), dma((2,)), dma((2, 5)), dma((2, 4)),
            ],
            compiler_params=pltpu.CompilerParams(collective_id=0, has_side_effects=True, vmem_limit_bytes=66_000_000),
            name="encoder",
        )(x_in.transpose(0, 2, 1), ln1_gain, ln2_gain, ln1_bias, ln2_bias, b_o, b_down, b_q, b_v, b_up,
          flat(w_q), flat(w_k), flat(w_v), w_o.reshape(layers, rows_q, half), w_up, w_down.transpose(0, 2, 1))
        return y_t.transpose(0, 2, 1)

    return jax.shard_map(local_fn, mesh=mesh, in_specs=in_specs, out_specs=act_spec, check_vma=False)
```
